128 devices in a mesh: gy: 32 (over y, x, core), gx: 4 (over z).
Axes of the slice: x: 4, y: 4, z: 4, core: 2. Of those that a mesh axis runs over, the one named last changes fastest.
Arguments:
- left_factor: bfloat16 [32768, 8192], P('gy', 'gx'), may hold values from -6 to 6
- right_factor: bfloat16 [8192, 8192], P('gy', 'gx'), may hold values from -0.0625 to 0.0625
Outputs:
- corrected: float32 [32768, 8192], P('gy', 'gx')
The draws below stay inside these ranges and needn't reach their ends.
All inputs are finite; a program needn't handle non-finite values.
Results may differ from the reference program's by a relative error of at most 0.0003.
Values may be sent and summed in bfloat16 or wider, within the bound.
No kernel may reach another device: no remote copies, remote signals or barrier semaphores. Data moves between devices by JAX's collectives and lax.ppermute only.
A program may use at most 192 MiB of HBM per device.

```python
import jax
import jax.numpy as jnp
from jax import lax

ROWS = 32768
COLS = 8192
INNER = 8192


def shard_levels(key, shape, shards, smallest, high):
    loudness, own = 1.0, jax.random.fold_in(key, 6)
    for dim, blocks in shards:
        steps = jnp.exp(jax.random.uniform(jax.random.fold_in(own, dim), (blocks,), jnp.float32, smallest / len(shards), high / len(shards)))
        loudness = loudness * jnp.repeat(steps, shape[dim] // blocks).reshape([-1 if axis == dim else 1 for axis in range(len(shape))])
    return loudness


def scatter_about(own_key, shape, spread, most, split=(), kind=jnp.bfloat16):
    drawn = spread * jax.random.normal(own_key, shape, jnp.float32)
    if split:
        drawn = drawn * shard_levels(own_key, shape, split, -0.22, 0.18)
    return jnp.clip(drawn, -most, most).astype(kind)


def setup_inputs(seed: int = 0) -> dict:
    splits = jax.random.split(jax.random.key(seed), 3)
    return {
        "left_factor": scatter_about(splits[0], (ROWS, INNER), 1.0, 6.0, ((0, 32), (1, 4))),
        "right_factor": scatter_about(splits[1], (INNER, COLS), INNER ** -0.5, 0.0625, ((0, 32), (1, 4))),
    }


def reference(left_factor, right_factor):
    corrected = jnp.dot(left_factor, right_factor, preferred_element_type=jnp.float32)
    row_power = lax.optimization_barrier(jnp.sum(corrected * corrected, axis=1))
    corrected = corrected * lax.rsqrt(row_power / COLS + 1e-06)[:, None]
    return corrected
```

```python
import jax
import jax.numpy as jnp
from jax import lax
from jax.sharding import PartitionSpec as P

ROW_CHUNKS = 4


def per_device(left, right):
    n = lax.axis_size("gx")
    up = [(i, (i + 1) % n) for i in range(n)]
    down = [(i, (i - 1) % n) for i in range(n)]
    z = lax.axis_index("gx")
    rows, depth = left.shape
    cols = right.shape[1]
    rc = rows // ROW_CHUNKS

    panel = lax.all_gather(right, "gy", axis=0, tiled=True)

    own = [left[i * rc:(i + 1) * rc] for i in range(ROW_CHUNKS)]
    below = [lax.ppermute(c, "gx", up) for c in own]
    above = [lax.ppermute(c, "gx", down) for c in own]
    far = [lax.ppermute(below[i], "gx", up) if i % 2 == 0 else lax.ppermute(above[i], "gx", down) for i in range(ROW_CHUNKS)]

    def times(block, rel):
        k = lax.rem(z + rel, n) * depth
        return jnp.dot(block, lax.dynamic_slice_in_dim(panel, k, depth, 0), preferred_element_type=jnp.float32)

    total = times(left, 0) + times(jnp.concatenate(below), n - 1) + times(jnp.concatenate(above), 1)
    total = total + times(jnp.concatenate(far), 2)
    power = lax.psum(jnp.sum(total * total, axis=1), "gx")
    return total * lax.rsqrt(power / (cols * n) + 1e-06)[:, None]


def solution(mesh):
    placed = (P("gy", "gx"), P("gy", "gx"))
    return jax.shard_map(per_device, mesh=mesh, in_specs=placed, out_specs=P("gy", "gx"), check_vma=False)
```

```python
import functools

import jax
import jax.numpy as jnp
from jax import lax
from jax.experimental import pallas as pl
from jax.experimental.pallas import tpu as pltpu
from jax.sharding import PartitionSpec as P


ROW_CHUNKS = 4
NX = NY = NZ = 4
NC = 2
MT, NT = 256, 512


def gy(y, x, c):
    return ((y % NY) * NX + x % NX) * NC + c


def along(axis, first):
    pairs = []
    for y in range(NY):
        for x in range(NX):
            for c in range(NC):
                step = 1 if (c == 0) == first else -1
                if axis == "x":
                    pairs.append((gy(y, x, c), gy(y, x + step, c)))
                elif axis == "y":
                    pairs.append((gy(y, x, c), gy(y + step, x, c)))
                elif axis == "core":
                    pairs.append((gy(y, x, c), gy(y, x, 1 - c)))
                else:
                    for z in range(NZ):
                        pairs.append((gy(y, x, c) * NZ + z, gy(y, x, c) * NZ + (z + step) % NZ))
    return pairs


def move(value, axis, first):
    name = ("gy", "gx") if axis == "z" else "gy"
    return lax.ppermute(value, name, along(axis, first))


def ring(value, axis):
    behind = move(value, axis, True)
    ahead = move(value, axis, False)
    return [value, behind, ahead, move(behind, axis, True)]


def offset(slot, core):
    back = jnp.where(core == 0, 3, 1)
    return (0, back, 4 - back, 2)[slot]


def slot_of(distance, core):
    near = jnp.where((distance == 3) == (core == 0), 1, 2)
    return jnp.where(distance == 0, 0, jnp.where(distance == 2, 3, near))


def load_tile(pos, pieces, h, kz, tile, sem):
    y0, x0, c0 = pos[0], pos[1], pos[2]
    distance = lax.rem(kz - y0 + 4, 4)
    step = tile.shape[0] // 8
    for q in range(2):
        core = c0 if q == 0 else 1 - c0
        at = slot_of(distance, core)
        for r in range(4):
            if h == 0:
                x = lax.rem(x0 + offset(r, core), 4)
                dst = tile.at[pl.ds(pl.multiple_of(x * 2 * step + core * step, step), step), :]
                for line in range(4):
                    @pl.when(at == line)
                    def _():
                        pltpu.make_async_copy(pieces[h][line][q].at[pl.ds(r * step, step), :], dst, sem).start()
            else:
                x = lax.rem(x0 + offset(r, core), 4)
                dst = tile.at[pl.ds(pl.multiple_of(x * 2 * step + core * step, step), step), :]
                src = pieces[h][r][q].at[pl.ds(pl.multiple_of(at * step, step), step), :]
                pltpu.make_async_copy(src, dst, sem).start()


def landed(ref, sem):
    pltpu.make_async_copy(ref, ref, sem).wait()


def nest(flat):
    return [[[flat[(h * 4 + line) * 2 + q] for q in range(2)] for line in range(4)] for h in range(2)]


def near_kernel(pos, left, *refs):
    behind, ahead, pieces, out = refs[:4], refs[4:8], nest(refs[8:24]), refs[24]
    a_v, t_v, o_v, a_sem, t_sem, o_sem = refs[25:]
    rows, _ = left.shape
    half = t_v.shape[2]
    rc = rows // ROW_CHUNKS
    z0, core = pos[3], pos[2]
    kz = [lax.rem(z0 + offset(b, core), 4) for b in range(3)]
    steps = [(h, b) for h in range(2) for b in range(3)]

    pltpu.make_async_copy(left, a_v.at[0], a_sem.at[0]).start()
    load_tile(pos, pieces, 0, kz[0], t_v.at[0], t_sem.at[0])
    for b, chunks in ((1, behind), (2, ahead)):
        for i, chunk in enumerate(chunks):
            pltpu.make_async_copy(chunk, a_v.at[b, pl.ds(i * rc, rc), :], a_sem.at[b]).start()
    for s, (h, b) in enumerate(steps):
        if s + 1 < len(steps):
            nh, nb = steps[s + 1]
            load_tile(pos, pieces, nh, kz[nb], t_v.at[(s + 1) % 2], t_sem.at[(s + 1) % 2])
        if h == 0:
            landed(a_v.at[b], a_sem.at[b])
        landed(t_v.at[s % 2], t_sem.at[s % 2])

        @pl.loop(0, (rows // MT) * (half // NT))
        def _(t):
            m = pl.multiple_of((t // (half // NT)) * MT, MT)
            n = pl.multiple_of((t % (half // NT)) * NT, NT)
            r = jnp.dot(a_v[b, pl.ds(m, MT), :], t_v[s % 2, :, pl.ds(n, NT)], preferred_element_type=jnp.float32)
            if b == 0:
                o_v[h, pl.ds(m, MT), pl.ds(n, NT)] = r
            else:
                o_v[h, pl.ds(m, MT), pl.ds(n, NT)] += r

        if b == 2:
            pltpu.make_async_copy(o_v.at[h], out.at[:, pl.ds(h * half, half)], o_sem.at[h]).start()
    for h in range(2):
        landed(o_v.at[h], o_sem.at[h])


def far_kernel(first, count, pos, near, *refs):
    chunks, pieces = refs[:count], nest(refs[count:count + 16])
    out, power, a_v, t_v, o_v, a_sem, t_sem, o_sem, w_sem = refs[count + 16:]
    rows = a_v.shape[0]
    rc = rows // count
    half = t_v.shape[2]
    kz = lax.rem(pos[3] + 2, 4)
    for i, chunk in enumerate(chunks):
        pltpu.make_async_copy(chunk, a_v.at[pl.ds(i * rc, rc), :], a_sem).start()
    for h in range(2):
        load_tile(pos, pieces, h, kz, t_v.at[h], t_sem.at[h])
        pltpu.make_async_copy(
            near.at[pl.ds(first * rc, rows), pl.ds(h * half, half)], o_v.at[h], o_sem.at[h]).start()
    landed(a_v, a_sem)
    for h in range(2):
        landed(t_v.at[h], t_sem.at[h])
        landed(o_v.at[h], o_sem.at[h])

        @pl.loop(0, (rows // MT) * (half // NT))
        def _(t):
            m = pl.multiple_of((t // (half // NT)) * MT, MT)
            n = pl.multiple_of((t % (half // NT)) * NT, NT)
            o_v[h, pl.ds(m, MT), pl.ds(n, NT)] += jnp.dot(
                a_v[pl.ds(m, MT), :], t_v[h, :, pl.ds(n, NT)], preferred_element_type=jnp.float32)

        pltpu.make_async_copy(o_v.at[h], out.at[:, pl.ds(h * half, half)], w_sem.at[h]).start()

    @pl.loop(0, rows // 128)
    def _(t):
        m = pl.multiple_of(t * 128, 128)
        lanes = jnp.zeros((128, 128), jnp.float32)
        for h in range(2):
            for n in range(half // 128):
                v = o_v[h, pl.ds(m, 128), pl.ds(n * 128, 128)]
                lanes = lanes + v * v
        power[:, pl.ds(m, 128)] = jnp.sum(lanes.T, axis=0, keepdims=True) + jnp.zeros((8, 128), jnp.float32)

    for h in range(2):
        landed(o_v.at[h], w_sem.at[h])


def scale_kernel(cols, value, p0, p1, p2, p3, *refs):
    out = refs[-1]
    total = (p0[0:1, :] + p1[0:1, :]) + (p2[0:1, :] + p3[0:1, :])
    factor = lax.rsqrt(total / cols + 1e-06)
    factor = jnp.broadcast_to(factor, (128, 128)).T[:, 0:1]
    out[...] = value[...] * factor


ANY = pl.BlockSpec(memory_space=pl.ANY)
SMEM = pl.BlockSpec(memory_space=pltpu.SMEM)


def near(pos, left, behind, ahead, pieces):
    rows, depth = left.shape
    half = pieces[0].shape[1]
    return pl.pallas_call(
        near_kernel,
        out_shape=jax.ShapeDtypeStruct((rows, 2 * half), jnp.float32),
        in_specs=[SMEM] + [ANY] * 25,
        out_specs=ANY,
        scratch_shapes=[
            pltpu.VMEM((3, rows, depth), left.dtype),
            pltpu.VMEM((2, depth, half), left.dtype),
            pltpu.VMEM((2, rows, half), jnp.float32),
            pltpu.SemaphoreType.DMA((3,)),
            pltpu.SemaphoreType.DMA((2,)),
            pltpu.SemaphoreType.DMA((2,)),
        ],
        cost_estimate=pl.CostEstimate(flops=2 * rows * 3 * depth * 2 * half, bytes_accessed=48 << 20, transcendentals=0),
        compiler_params=pltpu.CompilerParams(vmem_limit_bytes=48 << 20),
        name="near",
    )(pos, left, *behind, *ahead, *pieces)


def far(first, pos, base, chunks, pieces):
    rc, depth = chunks[0].shape
    rows = rc * len(chunks)
    half = pieces[0].shape[1]
    return pl.pallas_call(
        functools.partial(far_kernel, first, len(chunks)),
        out_shape=(jax.ShapeDtypeStruct((rows, 2 * half), jnp.float32), jax.ShapeDtypeStruct((8, rows), jnp.float32)),
        in_specs=[SMEM] + [ANY] * (1 + len(chunks) + 16),
        out_specs=(ANY, pl.BlockSpec(memory_space=pltpu.VMEM)),
        scratch_shapes=[
            pltpu.VMEM((rows, depth), chunks[0].dtype),
            pltpu.VMEM((2, depth, half), chunks[0].dtype),
            pltpu.VMEM((2, rows, half), jnp.float32),
            pltpu.SemaphoreType.DMA,
            pltpu.SemaphoreType.DMA((2,)),
            pltpu.SemaphoreType.DMA((2,)),
            pltpu.SemaphoreType.DMA((2,)),
        ],
        cost_estimate=pl.CostEstimate(flops=2 * rows * depth * 2 * half, bytes_accessed=24 << 20, transcendentals=0),
        compiler_params=pltpu.CompilerParams(vmem_limit_bytes=40 << 20),
    )(pos, base, *chunks, *pieces)


def scale(first, rows, cols, value, powers, base):
    count, width = value.shape
    extra = [] if base is None else [base]
    start = first // 128
    return pl.pallas_call(
        functools.partial(scale_kernel, cols),
        grid=(count // 128,),
        out_shape=jax.ShapeDtypeStruct((rows, width), jnp.float32),
        in_specs=[pl.BlockSpec((128, width), lambda i: (i, 0))] + [pl.BlockSpec((8, 128), lambda i: (0, i))] * 4 + [ANY] * len(extra),
        out_specs=pl.BlockSpec((128, width), lambda i: (start + i, 0)),
        input_output_aliases={5: 0} if extra else {},
        cost_estimate=pl.CostEstimate(flops=count * width * 30, bytes_accessed=8 * count * width, transcendentals=0),
        compiler_params=pltpu.CompilerParams(vmem_limit_bytes=16 << 20),
    )(value, *powers, *extra)


def per_device(left, right):
    rows, _ = left.shape
    width = right.shape[1]
    rc, half = rows // ROW_CHUNKS, width // 2
    me, z = lax.axis_index("gy"), lax.axis_index("gx")
    pos = jnp.stack([me // (NX * NC), (me // NC) % NX, me % NC, z]).astype(jnp.int32)

    lefts = [ring(left[i * rc:(i + 1) * rc], "z") for i in range(ROW_CHUNKS)]
    pieces = []
    for h, (a, b) in enumerate((("x", "y"), ("y", "x"))):
        line = jnp.concatenate(ring(right[:, h * half:(h + 1) * half], a), axis=0)
        for v in ring(line, b):
            pieces += [v, move(v, "core", True)]

    base = near(pos, left, [c[1] for c in lefts], [c[2] for c in lefts], pieces)
    out = None
    for first, last in ((0, 3), (3, 4)):
        value, power = far(first, pos, base, [c[3] for c in lefts[first:last]], pieces)
        around = [(i, (i + 2) % NZ) for i in range(NZ)]
        powers = [power, move(power, "z", True), move(power, "z", False)]
        powers.append(lax.ppermute(power, "gx", around))
        out = scale(first * rc, rows, width * NZ, value, powers, out)
    return out


def solution(mesh):
    placed = (P("gy", "gx"), P("gy", "gx"))
    return jax.shard_map(per_device, mesh=mesh, in_specs=placed, out_specs=P("gy", "gx"), check_vma=False)
```

```python
import functools

import jax
import jax.numpy as jnp
from jax import lax
from jax.experimental import pallas as pl
from jax.experimental.pallas import tpu as pltpu
from jax.sharding import PartitionSpec as P


ROW_CHUNKS = 4
NX = NY = NZ = 4
NC = 2
MT, NT = 512, 512

FAR_MIB = 6


def gy(y, x, c):
    return ((y % NY) * NX + x % NX) * NC + c


def along(axis, first):
    pairs = []
    for y in range(NY):
        for x in range(NX):
            for c in range(NC):
                step = 1 if (c == 0) == first else -1
                if axis == "x":
                    pairs.append((gy(y, x, c), gy(y, x + step, c)))
                elif axis == "y":
                    pairs.append((gy(y, x, c), gy(y + step, x, c)))
                elif axis == "core":
                    pairs.append((gy(y, x, c), gy(y, x, 1 - c)))
                else:
                    for z in range(NZ):
                        pairs.append((gy(y, x, c) * NZ + z, gy(y, x, c) * NZ + (z + step) % NZ))
    return pairs


def move(value, axis, first):
    name = ("gy", "gx") if axis == "z" else "gy"
    return lax.ppermute(value, name, along(axis, first))


def ring(value, axis):
    behind = move(value, axis, True)
    ahead = move(value, axis, False)
    return [value, behind, ahead, move(behind, axis, True)]


def exchange(power):
    opposite = lax.ppermute(power, "gx", [(i, (i + 2) % NZ) for i in range(NZ)])
    return [power, move(power, "z", True), move(power, "z", False), opposite]


def offset(slot, core):
    back = jnp.where(core == 0, 3, 1)
    return (0, back, 4 - back, 2)[slot]


def slot_of(distance, core):
    near = jnp.where((distance == 3) == (core == 0), 1, 2)
    return jnp.where(distance == 0, 0, jnp.where(distance == 2, 3, near))


def plan(pos):
    y0, core, z0 = pos[0], pos[2], pos[3]
    d = lax.rem(z0 - y0 + 4, 4)
    order = (
        jnp.where((d == 1) | (d == 2), 3, 0),
        jnp.where(d == 1, 0, 1),
        jnp.where(d == 2, 0, jnp.where(d == 1, 1, 3)),
    )
    where = []
    for b in range(3):
        distance = offset(b, core)
        where.append(jnp.where(distance == order[0], 0, jnp.where(distance == order[1], 1, 2)))
    return [lax.rem(z0 + o, 4) for o in order], where


def turned(x, x0):
    return lax.rem(x - x0 + 5, 4)


def copy_left_half(pos, pieces, n, y, lines, place, tile, sem):
    step = pieces[0][0][0].shape[0] // 4
    for q in range(2):
        core = pos[2] if q == 0 else 1 - pos[2]
        line = slot_of(lax.rem(y - pos[0] + 4, 4), core)
        to = [pl.multiple_of(place(lax.rem(offset(r, core) + 1, 4)) + core * step, step) for r in range(4)]
        for k in lines:
            @pl.when(line == k)
            def _():
                for r in range(4):
                    src = pieces[0][k][q].at[pl.ds(r * step, step), pl.ds(n, tile.shape[1])]
                    pltpu.make_async_copy(src, tile.at[pl.ds(to[r], step), :], sem).start()


def copy_right_half(pos, pieces, n, ys, lines, place, tile, sem):
    step = pieces[1][lines[0]][0].shape[0] // 4
    for q in range(2):
        core = pos[2] if q == 0 else 1 - pos[2]
        at = [pl.multiple_of(slot_of(lax.rem(y - pos[0] + 4, 4), core) * step, step) for y in ys]
        for k in lines:
            turn = lax.rem(offset(k, core) + 1, 4)
            for p in range(len(ys)):
                to = pl.multiple_of(place(p, turn) + core * step, step)
                src = pieces[1][k][q].at[pl.ds(at[p], step), pl.ds(n, tile.shape[1])]
                pltpu.make_async_copy(src, tile.at[pl.ds(to, step), :], sem).start()


def copy_left(sources, b, place, seg, dst, sem):
    for x in range(4):
        wanted, at = place(x)

        @pl.when(wanted)
        def _():
            col = pl.ds(pl.multiple_of(at, seg), seg)
            for i, chunk in enumerate(sources[b]):
                size = chunk.shape[0]
                pltpu.make_async_copy(chunk.at[:, pl.ds(x * seg, seg)], dst.at[pl.ds(i * size, size), col], sem).start()


def landed(ref, sem):
    pltpu.make_async_copy(ref, ref, sem).wait()


def nest(flat):
    return [[[flat[(h * 4 + line) * 2 + q] for q in range(2)] for line in range(4)] for h in range(2)]


def multiply(a_v, tile, acc, col, spans, add):
    rows, nt = a_v.shape[0], tile.shape[1]

    @pl.loop(0, rows // MT)
    def _(t):
        at = pl.ds(pl.multiple_of(t * MT, MT), MT)
        cols = pl.ds(col, nt)
        r = acc[at, cols] if add else None
        for a, b, size in spans:
            d = jnp.dot(a_v[at, pl.ds(a, size)], tile[pl.ds(b, size), :], preferred_element_type=jnp.float32)
            r = d if r is None else r + d
        acc[at, cols] = r


def left_kernel(pos, left, *refs):
    sources, lines = ([left], refs[:4], refs[4:8]), refs[8:14]
    acc, a_v, t_v, a_sem, t_sem = refs[14:]
    pieces = [[lines[2 * k:2 * k + 2] for k in range(3)]]
    _, depth = left.shape
    half, nt, seg, x0 = acc.shape[1] // 2, t_v.shape[2], depth // 4, pos[1]
    blocks, where = plan(pos)

    def fetch(s, p):
        copy_left_half(
            pos, pieces, s * nt, blocks[p], range(3), lambda t: (4 * p + t) * seg, t_v.at[s % 2], t_sem.at[s % 2, p])

    for b in range(3):
        copy_left(sources, b, lambda x: (where[b] < 2, (4 * where[b] + turned(x, x0)) * seg),
                  seg, a_v, a_sem.at[jnp.minimum(where[b], 1)])
        if b < 2:
            fetch(0, b)
    for s in range(half // nt):
        tile, col = t_v.at[s % 2], s * nt
        for p in range(2):
            if col + nt < half:
                fetch(s + 1, p)
        for p in range(2):
            if s == 0:
                landed(a_v.at[:, pl.ds(0, 4 * seg)], a_sem.at[p])
            landed(tile.at[pl.ds(0, 4 * seg), :], t_sem.at[s % 2, p])
            if s == 0:
                multiply(a_v, tile, acc, col, ((4 * p * seg, 4 * p * seg, 4 * seg),), p > 0)
        if s > 0:
            multiply(a_v, tile, acc, col, ((0, 0, 8 * seg),), False)


def right_kernel(pos, before, left, *refs):
    sources, lines = ([left], refs[:4], refs[4:8]), refs[8:14]
    acc, a_v, t_v, a_sem, t_sem = refs[14:]
    pieces = [None, [lines[2 * k:2 * k + 2] for k in range(3)]]
    _, depth = left.shape
    half, nt, seg, x0 = acc.shape[1] // 2, t_v.shape[2], depth // 4, pos[1]
    blocks, where = plan(pos)

    def fetch(s, p):
        copy_right_half(
            pos, pieces, s * nt, [blocks[p]], range(3), lambda _, t: (3 * p + t) * seg, t_v.at[s % 2], t_sem.at[s % 2, p])

    for b in range(3):
        copy_left(sources, b, lambda x: (turned(x, x0) < 3, (3 * where[b] + turned(x, x0)) * seg),
                  seg, a_v, a_sem.at[where[b]])
        fetch(0, b)
    for s in range(half // nt):
        tile, col = t_v.at[s % 2], half + s * nt
        for p in range(3):
            if (s + 1) * nt < half:
                fetch(s + 1, p)
        for p in range(3):
            if s == 0:
                landed(a_v.at[:, pl.ds(0, 3 * seg)], a_sem.at[p])
            landed(tile.at[pl.ds(0, 3 * seg), :], t_sem.at[s % 2, p])
            if s == 0:
                multiply(a_v, tile, acc, col, ((3 * p * seg, 3 * p * seg, 3 * seg),), p > 0)
        if s > 0:
            multiply(a_v, tile, acc, col, ((0, 0, 9 * seg),), False)


def rest_kernel(pos, before, left, *refs):
    sources, pieces = ([left], refs[:4], refs[4:8]), nest(refs[8:24])
    acc, far_v, a_v, t_v, a_sem, t_sem, f_sem = refs[24:]
    _, depth = left.shape
    half, nt, seg, x0 = acc.shape[1] // 2, t_v.shape[2], depth // 4, pos[1]
    blocks, where = plan(pos)
    parts = half // nt
    for s in range(parts):
        copy_left_half(
            pos, pieces, s * nt, blocks[2], range(4), lambda t: lax.rem(t + 1, 4) * seg, t_v.at[s], t_sem.at[s])
        if s == 0:
            for b in range(3):
                copy_left(sources, b, lambda x: (
                    (where[b] == 2) | (turned(x, x0) == 3),
                    jnp.where(turned(x, x0) == 3, where[b], 3 + turned(x, x0)) * seg), seg, a_v,
                    a_sem.at[jnp.where(where[b] == 2, 0, 1)])
    for s in range(parts):
        copy_right_half(
            pos, pieces, s * nt, blocks, (3,), lambda p, t: p * seg, t_v.at[parts + s], t_sem.at[parts + s])

    def place(t):
        return lax.rem(x0 + t + 3, 4) * seg

    opposite = lax.rem(pos[3] + 2, 4)
    for s in range(parts):
        copy_left_half(pos, pieces, s * nt, opposite, range(4), place, far_v.at[s], f_sem)
        copy_right_half(
            pos, pieces, s * nt, [opposite], range(4), lambda _, t: place(t), far_v.at[parts + s], f_sem)
    for s in range(2 * parts):
        if s == 0:
            landed(a_v.at[:, pl.ds(2 * seg, 4 * seg)], a_sem.at[0])
        if s == parts:
            landed(a_v.at[:, pl.ds(0, 2 * seg)], a_sem.at[1])
        first, size = (2 * seg, 4 * seg) if s < parts else (0, 3 * seg)
        landed(t_v.at[s, pl.ds(0, size), :], t_sem.at[s])
        multiply(a_v, t_v.at[s], acc, s * nt, ((first, 0, size),), True)
    landed(far_v, f_sem)


def far_multiply(low, mt, a_v, tile, acc, p_v, s):
    rows, nt = a_v.shape[0], tile.shape[1]

    @pl.loop(0, rows // mt)
    def _(t):
        at = pl.ds(pl.multiple_of(t * mt, mt), mt)
        to, cols = pl.ds(pl.multiple_of(low + t * mt, 128), mt), pl.ds(s * nt, nt)
        r = acc[to, cols] + jnp.dot(a_v[at, :], tile[...], preferred_element_type=jnp.float32)
        acc[to, cols] = r
        lanes = r[:, 0:128] * r[:, 0:128]
        for n in range(128, nt, 128):
            lanes = lanes + r[:, n:n + 128] * r[:, n:n + 128]
        p_v[at, :] = lanes if s == 0 else p_v[at, :] + lanes


def spread(p_v, power):
    for m in range(0, p_v.shape[0], 128):
        power[:, m:m + 128] = jnp.sum(p_v[m:m + 128, :].T, axis=0, keepdims=True) + jnp.zeros((8, 128), jnp.float32)


def far_kernel(low, before, t_in, *refs):
    count = len(refs) - 6
    chunks, (acc, t_v, power, a_v, p_v, a_sem) = refs[:count], refs[count:]
    rc = a_v.shape[0] // count
    for i, chunk in enumerate(chunks):
        pltpu.make_async_copy(chunk, a_v.at[pl.ds(i * rc, rc), :], a_sem).start()
    landed(a_v, a_sem)
    for s in range(t_v.shape[0]):
        far_multiply(low, min(256, a_v.shape[0]), a_v, t_in.at[s], acc, p_v, s)
    spread(p_v, power)


def scale_kernel(low, cols, acc, *refs):
    powers, (out, o_v, o_sem) = refs[:4], refs[-3:]
    size = o_v.shape[1]
    blocks = powers[0].shape[1] // size
    for i in range(blocks):
        if i >= 2:
            landed(o_v.at[i % 2], o_sem.at[i % 2])
        lanes = pl.ds(i * size, size)
        total = (powers[0][0:1, lanes] + powers[1][0:1, lanes]) + (powers[2][0:1, lanes] + powers[3][0:1, lanes])
        factor = jnp.broadcast_to(lax.rsqrt(total / cols + 1e-06), (size, size)).T[:, 0:1]
        o_v[i % 2] = acc[pl.ds(low + i * size, size), :] * factor
        pltpu.make_async_copy(o_v.at[i % 2], out.at[pl.ds(low + i * size, size), :], o_sem.at[i % 2]).start()
    for i in range(min(blocks, 2)):
        landed(o_v.at[i], o_sem.at[i])


ANY = pl.BlockSpec(memory_space=pltpu.HBM)
SMEM = pl.BlockSpec(memory_space=pltpu.SMEM)


VMEM = pl.BlockSpec(memory_space=pltpu.VMEM)


def kept(value):
    return pltpu.with_memory_space_constraint(value, pltpu.VMEM)


def apart(value):
    return pltpu.with_memory_space_constraint(value, pltpu.HBM)


def call(kernel, out_shape, in_specs, out_specs, scratch, flops, limit, aliases={}):
    return pl.pallas_call(
        kernel,
        out_shape=out_shape,
        in_specs=in_specs,
        out_specs=out_specs,
        scratch_shapes=scratch,
        input_output_aliases=aliases,
        cost_estimate=pl.CostEstimate(flops=flops, bytes_accessed=16 << 20, transcendentals=0),
        compiler_params=pltpu.CompilerParams(vmem_limit_bytes=limit << 20),
    )


def near(pos, left, behind, ahead, pieces):
    rows, depth = left.shape
    half, seg = pieces[0].shape[1], depth // 4
    total = pltpu.VMEM((rows, 2 * half), jnp.float32)
    flops = 2 * rows * half * seg
    dma = pltpu.SemaphoreType.DMA
    blocks = [left, *behind, *ahead]

    def scratch(size, depth, parts):
        return [pltpu.VMEM((rows, size), left.dtype), pltpu.VMEM((parts, depth, NT), left.dtype), dma((3,))]

    acc = call(
        left_kernel, total, [SMEM] + [ANY] * 15, VMEM, scratch(8 * seg, 8 * seg, 2) + [dma((2, 2))], 8 * flops, 18,
    )(pos, *blocks, *pieces[:6])
    acc = call(
        right_kernel, total, [SMEM, VMEM] + [ANY] * 15, VMEM, scratch(9 * seg, 9 * seg, 2) + [dma((2, 3))],
        9 * flops, 20, {1: 0},
    )(pos, kept(acc), *blocks, *pieces[8:14])
    parts = 2 * half // NT
    return call(
        rest_kernel, (total, pltpu.VMEM((parts, depth, NT), left.dtype)), [SMEM, VMEM] + [ANY] * 25, (VMEM, VMEM),
        scratch(6 * seg, depth, parts) + [dma((parts,)), dma], 7 * flops, 16, {1: 0},
    )(pos, kept(acc), *blocks, *pieces)


def far(low, acc, tile, chunks):
    rc, depth = chunks[0].shape
    rows = rc * len(chunks)
    out = pltpu.VMEM(acc.shape, acc.dtype), pltpu.VMEM(tile.shape, tile.dtype), jax.ShapeDtypeStruct((8, rows), jnp.float32)
    return call(
        functools.partial(far_kernel, low), out, [VMEM, VMEM] + [ANY] * len(chunks), (VMEM, VMEM, VMEM),
        [pltpu.VMEM((rows, depth), chunks[0].dtype), pltpu.VMEM((rows, 128), jnp.float32), pltpu.SemaphoreType.DMA],
        2 * rows * depth * acc.shape[1], FAR_MIB, {0: 0, 1: 1},
    )(kept(acc), kept(tile), *chunks)


def scale(low, cols, acc, powers, base):
    extra = [] if base is None else [base]
    return call(
        functools.partial(scale_kernel, low, cols), jax.ShapeDtypeStruct(acc.shape, jnp.float32),
        [VMEM] * 5 + [ANY] * len(extra), ANY,
        [pltpu.VMEM((2, 128, acc.shape[1]), jnp.float32), pltpu.SemaphoreType.DMA((2,))],
        powers[0].shape[1] * acc.shape[1] * 30, FAR_MIB, {5: 0} if extra else {},
    )(kept(acc), *powers, *extra)


def per_device(left, right):
    rows, _ = left.shape
    width = right.shape[1]
    rc, half = rows // ROW_CHUNKS, width // 2
    me, z = lax.axis_index("gy"), lax.axis_index("gx")
    pos = jnp.stack([me // (NX * NC), (me // NC) % NX, me % NC, z]).astype(jnp.int32)

    head, left_too = lax.optimization_barrier((left[:rc], left))
    lefts = [ring(left_too[i * rc:(i + 1) * rc] if i else head, "z") for i in range(ROW_CHUNKS)]
    pieces = []
    for h, (a, b) in enumerate((("x", "y"), ("y", "x"))):
        line = jnp.concatenate(ring(right[:, h * half:(h + 1) * half], a), axis=0)
        for v in ring(line, b):
            pieces += [v, move(v, "core", True)]

    pieces = [apart(v) for v in pieces]
    sides = [[apart(c[k]) for c in lefts] for k in (1, 2)]
    acc, tile = near(pos, apart(left), *sides, pieces)
    low = rows - rc
    acc, tile, power = far(0, acc, tile, [c[3] for c in lefts[:-1]])
    first = exchange(power)
    acc, tile, power = far(low, acc, tile, [lefts[-1][3]])
    second = exchange(power)
    return scale(low, width * NZ, acc, second, scale(0, width * NZ, acc, first, None))


def solution(mesh):
    placed = (P("gy", "gx"), P("gy", "gx"))
    return jax.shard_map(per_device, mesh=mesh, in_specs=placed, out_specs=P("gy", "gx"), check_vma=False)
```

```python
import functools

import jax
import jax.numpy as jnp
from jax import lax
from jax.experimental import pallas as pl
from jax.experimental.pallas import tpu as pltpu
from jax.sharding import PartitionSpec as P


ROW_CHUNKS = (384, 384, 256)
NX = NY = NZ = 4
NC = 2
MT, NT = 512, 512

NEAR_MIB, FAR_MIB = 11, 6


def gy(y, x, c):
    return ((y % NY) * NX + x % NX) * NC + c


def along(axis, first):
    pairs = []
    for y in range(NY):
        for x in range(NX):
            for c in range(NC):
                step = 1 if (c == 0) == first else -1
                if axis == "x":
                    pairs.append((gy(y, x, c), gy(y, x + step, c)))
                elif axis == "y":
                    pairs.append((gy(y, x, c), gy(y + step, x, c)))
                elif axis == "core":
                    pairs.append((gy(y, x, c), gy(y, x, 1 - c)))
                else:
                    for z in range(NZ):
                        pairs.append((gy(y, x, c) * NZ + z, gy(y, x, c) * NZ + (z + step) % NZ))
    return pairs


def move(value, axis, first):
    name = ("gy", "gx") if axis == "z" else "gy"
    return lax.ppermute(value, name, along(axis, first))


def ring(value, axis):
    behind = move(value, axis, True)
    ahead = move(value, axis, False)
    return [value, behind, ahead, move(behind, axis, True)]


def exchange(power):
    opposite = lax.ppermute(power, "gx", [(i, (i + 2) % NZ) for i in range(NZ)])
    return [power, move(power, "z", True), move(power, "z", False), opposite]


def offset(slot, core):
    back = jnp.where(core == 0, 3, 1)
    return (0, back, 4 - back, 2)[slot]


def slot_of(distance, core):
    near = jnp.where((distance == 3) == (core == 0), 1, 2)
    return jnp.where(distance == 0, 0, jnp.where(distance == 2, 3, near))


def plan(pos):
    y0, core, z0 = pos[0], pos[2], pos[3]
    d = lax.rem(z0 - y0 + 4, 4)
    order = (
        jnp.where((d == 1) | (d == 2), 3, 0),
        jnp.where(d == 1, 0, 1),
        jnp.where(d == 2, 0, jnp.where(d == 1, 1, 3)),
    )
    where = []
    for b in range(3):
        distance = offset(b, core)
        where.append(jnp.where(distance == order[0], 0, jnp.where(distance == order[1], 1, 2)))
    return [lax.rem(z0 + o, 4) for o in order], where


def turned(x, x0):
    return lax.rem(x - x0 + 5, 4)


def copy_left_half(pos, pieces, n, y, lines, place, tile, sem):
    step = pieces[0][0][0].shape[0] // 4
    for q in range(2):
        core = pos[2] if q == 0 else 1 - pos[2]
        line = slot_of(lax.rem(y - pos[0] + 4, 4), core)
        to = [pl.multiple_of(place(lax.rem(offset(r, core) + 1, 4)) + core * step, step) for r in range(4)]
        for k in lines:
            @pl.when(line == k)
            def _():
                for r in range(4):
                    src = pieces[0][k][q].at[pl.ds(r * step, step), pl.ds(n, tile.shape[1])]
                    pltpu.make_async_copy(src, tile.at[pl.ds(to[r], step), :], sem).start()


def copy_right_half(pos, pieces, n, ys, lines, place, tile, sem):
    step = pieces[1][lines[0]][0].shape[0] // 4
    for q in range(2):
        core = pos[2] if q == 0 else 1 - pos[2]
        at = [pl.multiple_of(slot_of(lax.rem(y - pos[0] + 4, 4), core) * step, step) for y in ys]
        for k in lines:
            turn = lax.rem(offset(k, core) + 1, 4)
            for p in range(len(ys)):
                to = pl.multiple_of(place(p, turn) + core * step, step)
                src = pieces[1][k][q].at[pl.ds(at[p], step), pl.ds(n, tile.shape[1])]
                pltpu.make_async_copy(src, tile.at[pl.ds(to, step), :], sem).start()


def copy_left(sources, b, place, seg, dst, sem):
    for x in range(4):
        col = pl.ds(pl.multiple_of(place(x), seg), seg)
        low = 0
        for chunk in sources[b]:
            to = dst.at[pl.ds(low, chunk.shape[0]), col]
            pltpu.make_async_copy(chunk.at[:, pl.ds(x * seg, seg)], to, sem).start()
            low += chunk.shape[0]


def landed(ref, sem):
    pltpu.make_async_copy(ref, ref, sem).wait()


def nest(flat):
    return [[[flat[(h * 4 + line) * 2 + q] for q in range(2)] for line in range(4)] for h in range(2)]


def spot(p, t, seg):
    return jnp.where(t == 3, jnp.where(p == 2, 11, p), 2 + 3 * p + t) * seg


def multiply(a_v, tile, acc, col, spans, add):
    rows, nt = a_v.shape[0], tile.shape[1]

    @pl.loop(0, rows // MT)
    def _(t):
        at = pl.ds(pl.multiple_of(t * MT, MT), MT)
        cols = pl.ds(col, nt)
        r = acc[at, cols] if add else None
        for a, b, size in spans:
            d = jnp.dot(a_v[at, pl.ds(a, size)], tile[pl.ds(b, size), :], preferred_element_type=jnp.float32)
            r = d if r is None else r + d
        acc[at, cols] = r


def left_kernel(pos, left, *refs):
    count = len(ROW_CHUNKS)
    sources, lines = ([left], refs[:count], refs[count:count + 1]), refs[count + 1:count + 7]
    acc, a_v, t_v, a_sem, t_sem = refs[count + 7:]
    pieces = [[lines[2 * k:2 * k + 2] for k in range(3)]]
    _, depth = left.shape
    half, nt, seg, x0 = acc.shape[1] // 2, t_v.shape[2], depth // 4, pos[1]
    blocks, where = plan(pos)

    def fetch(s):
        for p in range(2):
            copy_left_half(
                pos, pieces, s * nt, blocks[p], range(3), lambda t: spot(p, t, seg), t_v.at[s % 2], t_sem.at[s % 2, p])

    for b in range(3):
        copy_left(sources, b, lambda x: spot(where[b], turned(x, x0), seg), seg, a_v, a_sem.at[where[b]])
        if b == 0:
            fetch(0)
    for s in range(half // nt):
        if (s + 1) * nt < half:
            fetch(s + 1)
        for p in range(2):
            if s == 0:
                landed(a_v.at[:, pl.ds(0, 4 * seg)], a_sem.at[p])
            landed(t_v.at[s % 2, pl.ds(0, 4 * seg), :], t_sem.at[s % 2, p])
            if s == 0:
                one, three = p * seg, (2 + 3 * p) * seg
                multiply(a_v, t_v.at[0], acc, 0, ((one, one, seg), (three, three, 3 * seg)), p > 0)
        if s > 0:
            multiply(a_v, t_v.at[s % 2], acc, s * nt, ((0, 0, 8 * seg),), False)
    landed(a_v.at[:, pl.ds(0, 4 * seg)], a_sem.at[2])


def right_kernel(pos, a_v, before, *refs):
    lines, (acc, _, t_v, t_sem) = refs[:6], refs[6:]
    pieces = [None, [lines[2 * k:2 * k + 2] for k in range(3)]]
    half, nt, seg = acc.shape[1] // 2, t_v.shape[2], a_v.shape[1] // 12
    blocks, _ = plan(pos)

    def fetch(s, p):
        copy_right_half(
            pos, pieces, s * nt, [blocks[p]], range(3), lambda _, t: (3 * p + t) * seg, t_v.at[s % 2], t_sem.at[s % 2, p])

    for p in range(3):
        fetch(0, p)
    for s in range(half // nt):
        for p in range(3):
            if (s + 1) * nt < half:
                fetch(s + 1, p)
        for p in range(3):
            landed(t_v.at[s % 2, pl.ds(0, 3 * seg), :], t_sem.at[s % 2, p])
            if s == 0:
                multiply(a_v, t_v.at[0], acc, half, (((2 + 3 * p) * seg, 3 * p * seg, 3 * seg),), p > 0)
        if s > 0:
            multiply(a_v, t_v.at[s % 2], acc, half + s * nt, ((2 * seg, 0, 9 * seg),), False)


def rest_kernel(pos, a_v, before, *refs):
    pieces, (acc, far_v, t_v, t_sem, f_sem) = nest(refs[:16]), refs[16:]
    half, nt, seg = acc.shape[1] // 2, t_v.shape[2], a_v.shape[1] // 12
    blocks, _ = plan(pos)
    parts = half // nt
    for s in range(parts):
        copy_left_half(pos, pieces, s * nt, blocks[2], range(4), lambda t: t * seg, t_v.at[s], t_sem.at[s])
    for s in range(parts):
        copy_right_half(
            pos, pieces, s * nt, blocks, (3,), lambda p, t: p * seg, t_v.at[parts + s], t_sem.at[parts + s])

    def place(t):
        return lax.rem(pos[1] + t + 3, 4) * seg

    opposite = lax.rem(pos[3] + 2, 4)
    for s in range(parts):
        copy_left_half(pos, pieces, s * nt, opposite, range(4), place, far_v.at[s], f_sem)
        copy_right_half(
            pos, pieces, s * nt, [opposite], range(4), lambda _, t: place(t), far_v.at[parts + s], f_sem)
    for s in range(2 * parts):
        size = (4 if s < parts else 3) * seg
        landed(t_v.at[s, pl.ds(0, size), :], t_sem.at[s])
        spans = ((8 * seg, 0, 4 * seg),) if s < parts else ((0, 0, 2 * seg), (11 * seg, 2 * seg, seg))
        multiply(a_v, t_v.at[s], acc, s * nt, spans, True)
    landed(far_v, f_sem)


def far_multiply(low, mt, a_v, tile, acc, p_v, s):
    rows, nt = a_v.shape[0], tile.shape[1]

    @pl.loop(0, rows // mt)
    def _(t):
        at = pl.ds(pl.multiple_of(t * mt, mt), mt)
        to, cols = pl.ds(pl.multiple_of(low + t * mt, 128), mt), pl.ds(s * nt, nt)
        r = acc[to, cols] + jnp.dot(a_v[at, :], tile[...], preferred_element_type=jnp.float32)
        acc[to, cols] = r
        lanes = r[:, 0:128] * r[:, 0:128]
        for n in range(128, nt, 128):
            lanes = lanes + r[:, n:n + 128] * r[:, n:n + 128]
        p_v[at, :] = lanes if s == 0 else p_v[at, :] + lanes


def spread(p_v, power):
    for m in range(0, p_v.shape[0], 128):
        power[:, m:m + 128] = jnp.sum(p_v[m:m + 128, :].T, axis=0, keepdims=True) + jnp.zeros((8, 128), jnp.float32)


def far_kernel(low, before, t_in, *refs):
    chunks, (acc, t_v, power, a_v, p_v, a_sem) = refs[:-6], refs[-6:]
    at = 0
    for chunk in chunks:
        pltpu.make_async_copy(chunk, a_v.at[pl.ds(at, chunk.shape[0]), :], a_sem).start()
        at += chunk.shape[0]
    landed(a_v, a_sem)
    for s in range(t_v.shape[0]):
        far_multiply(low, min(256, a_v.shape[0]), a_v, t_in.at[s], acc, p_v, s)
    spread(p_v, power)


def scale_kernel(low, cols, acc, *refs):
    powers, (out, o_v, o_sem) = refs[:4], refs[-3:]
    size = o_v.shape[1]
    blocks = powers[0].shape[1] // size
    for i in range(blocks):
        if i >= 2:
            landed(o_v.at[i % 2], o_sem.at[i % 2])
        lanes = pl.ds(i * size, size)
        total = (powers[0][0:1, lanes] + powers[1][0:1, lanes]) + (powers[2][0:1, lanes] + powers[3][0:1, lanes])
        factor = jnp.broadcast_to(lax.rsqrt(total / cols + 1e-06), (size, size)).T[:, 0:1]
        o_v[i % 2] = acc[pl.ds(low + i * size, size), :] * factor
        pltpu.make_async_copy(o_v.at[i % 2], out.at[pl.ds(low + i * size, size), :], o_sem.at[i % 2]).start()
    for i in range(min(blocks, 2)):
        landed(o_v.at[i], o_sem.at[i])


ANY = pl.BlockSpec(memory_space=pltpu.HBM)
SMEM = pl.BlockSpec(memory_space=pltpu.SMEM)


VMEM = pl.BlockSpec(memory_space=pltpu.VMEM)


def kept(value):
    return pltpu.with_memory_space_constraint(value, pltpu.VMEM)


def apart(value):
    return pltpu.with_memory_space_constraint(value, pltpu.HBM)


def call(kernel, out_shape, in_specs, out_specs, scratch, flops, limit, aliases={}):
    return pl.pallas_call(
        kernel,
        out_shape=out_shape,
        in_specs=in_specs,
        out_specs=out_specs,
        scratch_shapes=scratch,
        input_output_aliases=aliases,
        cost_estimate=pl.CostEstimate(flops=flops, bytes_accessed=16 << 20, transcendentals=0),
        compiler_params=pltpu.CompilerParams(vmem_limit_bytes=limit << 20),
    )


def near(pos, left, behind, ahead, pieces):
    rows, depth = left.shape
    half, seg = pieces[0].shape[1], depth // 4
    total = pltpu.VMEM((rows, 2 * half), jnp.float32)
    flops = 2 * rows * half * seg
    dma = pltpu.SemaphoreType.DMA
    acc, blocks = call(
        left_kernel, (total, pltpu.VMEM((rows, 12 * seg), left.dtype)), [SMEM] + [ANY] * (8 + len(ROW_CHUNKS)), (VMEM, VMEM),
        [pltpu.VMEM((2, 8 * seg, NT), left.dtype), dma((3,)), dma((2, 2))], 8 * flops, NEAR_MIB,
    )(pos, left, *behind, ahead, *pieces[:6])
    acc, blocks = call(
        right_kernel, (total, pltpu.VMEM(blocks.shape, blocks.dtype)), [SMEM, VMEM, VMEM] + [ANY] * 6, (VMEM, VMEM),
        [pltpu.VMEM((2, 9 * seg, NT), left.dtype), dma((2, 3))], 9 * flops, NEAR_MIB, {1: 1, 2: 0},
    )(pos, kept(blocks), kept(acc), *pieces[8:14])
    parts = 2 * half // NT
    return call(
        rest_kernel, (total, pltpu.VMEM((parts, depth, NT), left.dtype)), [SMEM, VMEM, VMEM] + [ANY] * 16, (VMEM, VMEM),
        [pltpu.VMEM((parts, depth, NT), left.dtype), dma((parts,)), dma], 7 * flops, NEAR_MIB, {2: 0},
    )(pos, kept(blocks), kept(acc), *pieces)


def far(low, acc, tile, chunks):
    depth = chunks[0].shape[1]
    rows = sum(chunk.shape[0] for chunk in chunks)
    out = pltpu.VMEM(acc.shape, acc.dtype), pltpu.VMEM(tile.shape, tile.dtype), jax.ShapeDtypeStruct((8, rows), jnp.float32)
    return call(
        functools.partial(far_kernel, low), out, [VMEM, VMEM] + [ANY] * len(chunks), (VMEM, VMEM, VMEM),
        [pltpu.VMEM((rows, depth), chunks[0].dtype), pltpu.VMEM((rows, 128), jnp.float32), pltpu.SemaphoreType.DMA],
        2 * rows * depth * acc.shape[1], FAR_MIB, {0: 0, 1: 1},
    )(kept(acc), kept(tile), *chunks)


def scale(low, cols, acc, powers, base):
    extra = [] if base is None else [base]
    return call(
        functools.partial(scale_kernel, low, cols), jax.ShapeDtypeStruct(acc.shape, jnp.float32),
        [VMEM] * 5 + [ANY] * len(extra), ANY,
        [pltpu.VMEM((2, 128, acc.shape[1]), jnp.float32), pltpu.SemaphoreType.DMA((2,))],
        powers[0].shape[1] * acc.shape[1] * 30, FAR_MIB, {5: 0} if extra else {},
    )(kept(acc), *powers, *extra)


def per_device(left, right):
    rows, _ = left.shape
    width = right.shape[1]
    half = width // 2
    me, z = lax.axis_index("gy"), lax.axis_index("gx")
    pos = jnp.stack([me // (NX * NC), (me // NC) % NX, me % NC, z]).astype(jnp.int32)

    ahead = move(left, "z", False)
    behind, opposite, low = [], [], 0
    for i, size in enumerate(ROW_CHUNKS):
        behind.append(move(left[low:low + size], "z", True))
        opposite.append(move(behind[i], "z", True))
        low += size
    pieces = []
    for h, (a, b) in enumerate((("x", "y"), ("y", "x"))):
        line = jnp.concatenate(ring(right[:, h * half:(h + 1) * half], a), axis=0)
        for v in ring(line, b):
            pieces += [v, move(v, "core", True)]

    pieces = [apart(v) for v in pieces]
    acc, tile = near(pos, apart(left), [apart(v) for v in behind], apart(ahead), pieces)
    low = rows - ROW_CHUNKS[-1]
    acc, tile, power = far(0, acc, tile, opposite[:-1])
    first = exchange(power)
    acc, tile, power = far(low, acc, tile, opposite[-1:])
    second = exchange(power)
    return scale(low, width * NZ, acc, second, scale(0, width * NZ, acc, first, None))


def solution(mesh):
    placed = (P("gy", "gx"), P("gy", "gx"))
    return jax.shard_map(per_device, mesh=mesh, in_specs=placed, out_specs=P("gy", "gx"), check_vma=False)
```

```python
import functools

import jax
import jax.numpy as jnp
from jax import lax
from jax.experimental import pallas as pl
from jax.experimental.pallas import tpu as pltpu
from jax.sharding import PartitionSpec as P


ROW_CHUNKS = (384, 384, 256)
NX = NY = NZ = 4
NC = 2
NT = 512

NEAR_MIB, FAR_MIB = 11, 6


def gy(y, x, c):
    return ((y % NY) * NX + x % NX) * NC + c


def along(axis, first):
    pairs = []
    for y in range(NY):
        for x in range(NX):
            for c in range(NC):
                step = 1 if (c == 0) == first else -1
                if axis == "x":
                    pairs.append((gy(y, x, c), gy(y, x + step, c)))
                elif axis == "y":
                    pairs.append((gy(y, x, c), gy(y + step, x, c)))
                elif axis == "core":
                    pairs.append((gy(y, x, c), gy(y, x, 1 - c)))
                else:
                    for z in range(NZ):
                        pairs.append((gy(y, x, c) * NZ + z, gy(y, x, c) * NZ + (z + step) % NZ))
    return pairs


def move(value, axis, first):
    name = ("gy", "gx") if axis == "z" else "gy"
    return lax.ppermute(value, name, along(axis, first))


def ring(value, axis):
    behind = move(value, axis, True)
    ahead = move(value, axis, False)
    return [value, behind, ahead, move(behind, axis, True)]


def exchange(power):
    opposite = lax.ppermute(power, "gx", [(i, (i + 2) % NZ) for i in range(NZ)])
    return [power, move(power, "z", True), move(power, "z", False), opposite]


def offset(slot, core):
    back = jnp.where(core == 0, 3, 1)
    return (0, back, 4 - back, 2)[slot]


def slot_of(distance, core):
    near = jnp.where((distance == 3) == (core == 0), 1, 2)
    return jnp.where(distance == 0, 0, jnp.where(distance == 2, 3, near))


def plan(pos):
    y0, core, z0 = pos[0], pos[2], pos[3]
    d = lax.rem(z0 - y0 + 4, 4)
    order = (
        jnp.where((d == 1) | (d == 2), 3, 0),
        jnp.where(d == 1, 0, 1),
        jnp.where(d == 2, 0, jnp.where(d == 1, 1, 3)),
    )
    where = []
    for b in range(3):
        distance = offset(b, core)
        where.append(jnp.where(distance == order[0], 0, jnp.where(distance == order[1], 1, 2)))
    return [lax.rem(z0 + o, 4) for o in order], where


def turned(x, x0):
    return lax.rem(x - x0 + 5, 4)


def copy_left_half(pos, pieces, n, y, lines, place, tile, sem):
    step = pieces[0][0][0].shape[0] // 4
    for q in range(2):
        core = pos[2] if q == 0 else 1 - pos[2]
        line = slot_of(lax.rem(y - pos[0] + 4, 4), core)
        to = [pl.multiple_of(place(lax.rem(offset(r, core) + 1, 4)) + core * step, step) for r in range(4)]
        for k in lines:
            @pl.when(line == k)
            def _():
                for r in range(4):
                    src = pieces[0][k][q].at[pl.ds(r * step, step), pl.ds(n, tile.shape[1])]
                    pltpu.make_async_copy(src, tile.at[pl.ds(to[r], step), :], sem).start()


def copy_right_half(pos, pieces, n, ys, lines, place, tile, sem):
    step = pieces[1][lines[0]][0].shape[0] // 4
    for q in range(2):
        core = pos[2] if q == 0 else 1 - pos[2]
        at = [pl.multiple_of(slot_of(lax.rem(y - pos[0] + 4, 4), core) * step, step) for y in ys]
        for k in lines:
            turn = lax.rem(offset(k, core) + 1, 4)
            for p in range(len(ys)):
                to = pl.multiple_of(place(p, turn) + core * step, step)
                src = pieces[1][k][q].at[pl.ds(at[p], step), pl.ds(n, tile.shape[1])]
                pltpu.make_async_copy(src, tile.at[pl.ds(to, step), :], sem).start()


def copy_left(chunks, low, place, seg, dst, sem):
    for chunk in chunks:
        rows = pl.ds(low, chunk.shape[0])
        for x in range(4):
            col = pl.ds(pl.multiple_of(place(x), seg), seg)
            pltpu.make_async_copy(chunk.at[:, pl.ds(x * seg, seg)], dst.at[rows, col], sem).start()
        low += chunk.shape[0]


def landed(ref, sem):
    pltpu.make_async_copy(ref, ref, sem).wait()


def nest(flat):
    return [[[flat[(h * 4 + line) * 2 + q] for q in range(2)] for line in range(4)] for h in range(2)]


def spot(p, t, seg):
    return jnp.where(t == 3, jnp.where(p == 2, 11, p), 2 + 3 * p + t) * seg


def multiply(a_v, tile, acc, col, spans, add, low=0, high=None):
    rows, nt = (high or a_v.shape[0]) - low, tile.shape[1]
    mt = max(m for m in (512, 384, 256) if rows % m == 0)

    @pl.loop(0, rows // mt)
    def _(t):
        at = pl.ds(pl.multiple_of(low + t * mt, 128), mt)
        cols = pl.ds(col, nt)
        r = acc[at, cols] if add else None
        for a, b, size in spans:
            d = jnp.dot(a_v[at, pl.ds(a, size)], tile[pl.ds(b, size), :], preferred_element_type=jnp.float32)
            r = d if r is None else r + d
        acc[at, cols] = r


def left_tiles(pos, lines, blocks, nt, seg, t_v, t_sem):
    pieces = [[lines[2 * k:2 * k + 2] for k in range(3)]]

    def fetch(s, p):
        copy_left_half(
            pos, pieces, s * nt, blocks[p], range(3), lambda t: spot(p, t, seg), t_v.at[s % 2], t_sem.at[s % 2, p])

    return fetch


def left_kernel(low, pos, left, *refs):
    (first, second, side), lines, (acc, a_v, t_v, a_sem, t_sem) = refs[:3], refs[3:9], refs[9:]
    sources = [left.at[pl.ds(0, low), :]], [first, second], [side]
    half, nt, seg = acc.shape[1] // 2, t_v.shape[2], a_v.shape[1] // 12
    blocks, where = plan(pos)
    fetch = left_tiles(pos, lines, blocks, nt, seg, t_v, t_sem)
    for p in range(2):
        for b in range(3):
            @pl.when(where[b] == p)
            def _():
                copy_left(sources[b], 0, lambda x: spot(p, turned(x, pos[1]), seg), seg, a_v, a_sem.at[p])
        fetch(0, p)
    for s in range(half // nt):
        for p in range(2):
            if (s + 1) * nt < half:
                fetch(s + 1, p)
        for p in range(2):
            if s == 0:
                landed(a_v.at[pl.ds(0, low), pl.ds(0, 4 * seg)], a_sem.at[p])
            landed(t_v.at[s % 2, pl.ds(0, 4 * seg), :], t_sem.at[s % 2, p])
            if s == 0:
                one, three = p * seg, (2 + 3 * p) * seg
                multiply(a_v, t_v.at[0], acc, 0, ((one, one, seg), (three, three, 3 * seg)), p > 0, 0, low)
        if s > 0:
            multiply(a_v, t_v.at[s % 2], acc, s * nt, ((0, 0, 8 * seg),), False, 0, low)


def right_kernel(low, pos, a_in, before, left, *refs):
    chunks, lines, (acc, a_v, t_v, a_sem, t_sem) = refs[:5], refs[5:11], refs[11:]
    rows = left.shape[0]
    upper = [left.at[pl.ds(0, low), :]], chunks[:2], chunks[3:4]
    lower = [left.at[pl.ds(low, rows - low), :]], chunks[2:3], chunks[4:]
    pieces = [None, [lines[2 * k:2 * k + 2] for k in range(3)]]
    half, nt, seg = acc.shape[1] // 2, t_v.shape[2], a_v.shape[1] // 12
    blocks, where = plan(pos)

    def fetch(s, p):
        copy_right_half(
            pos, pieces, s * nt, [blocks[p]], range(3), lambda _, t: (3 * p + t) * seg, t_v.at[s % 2], t_sem.at[s % 2, p])

    fetch(0, 0)
    for b in range(3):
        copy_left(lower[b], low, lambda x: spot(where[b], turned(x, pos[1]), seg), seg, a_v, a_sem.at[0])
    for p in range(1, 3):
        fetch(0, p)
    for b in range(3):
        @pl.when(where[b] == 2)
        def _():
            copy_left(upper[b], 0, lambda x: spot(2, turned(x, pos[1]), seg), seg, a_v, a_sem.at[1])
    for s in range(half // nt):
        for p in range(3):
            if (s + 1) * nt < half:
                fetch(s + 1, p)
        for p in range(3):
            if (s, p) == (0, 0):
                landed(a_v.at[pl.ds(low, rows - low), :], a_sem.at[0])
            if (s, p) == (0, 2):
                landed(a_v.at[pl.ds(0, low), pl.ds(0, 4 * seg)], a_sem.at[1])
            landed(t_v.at[s % 2, pl.ds(0, 3 * seg), :], t_sem.at[s % 2, p])
            if s == 0:
                multiply(a_v, t_v.at[0], acc, half, (((2 + 3 * p) * seg, 3 * p * seg, 3 * seg),), p > 0)
        if s > 0:
            multiply(a_v, t_v.at[s % 2], acc, half + s * nt, ((2 * seg, 0, 9 * seg),), False)


def tail_kernel(low, pos, a_in, before, *refs):
    lines, (acc, a_v, t_v, t_sem) = refs[:6], refs[6:]
    half, nt, seg = acc.shape[1] // 2, t_v.shape[2], a_v.shape[1] // 12
    blocks, _ = plan(pos)
    fetch = left_tiles(pos, lines, blocks, nt, seg, t_v, t_sem)
    for s in range(half // nt):
        for p in range(2):
            fetch(s, p)
    for s in range(half // nt):
        for p in range(2):
            landed(t_v.at[s, pl.ds(0, 4 * seg), :], t_sem.at[s, p])
            one, three = p * seg, (2 + 3 * p) * seg
            multiply(a_v, t_v.at[s], acc, s * nt, ((one, one, seg), (three, three, 3 * seg)), p > 0, low)


def rest_kernel(pos, a_v, before, *refs):
    pieces, (acc, far_v, t_v, t_sem, f_sem) = nest(refs[:16]), refs[16:]
    half, nt, seg = acc.shape[1] // 2, t_v.shape[2], a_v.shape[1] // 12
    blocks, _ = plan(pos)
    parts = half // nt
    for s in range(parts):
        copy_left_half(pos, pieces, s * nt, blocks[2], range(4), lambda t: t * seg, t_v.at[s], t_sem.at[s])
    for s in range(parts):
        copy_right_half(
            pos, pieces, s * nt, blocks, (3,), lambda p, t: p * seg, t_v.at[parts + s], t_sem.at[parts + s])

    def place(t):
        return lax.rem(pos[1] + t + 3, 4) * seg

    opposite = lax.rem(pos[3] + 2, 4)
    for s in range(parts):
        copy_left_half(pos, pieces, s * nt, opposite, range(4), place, far_v.at[s], f_sem)
        copy_right_half(
            pos, pieces, s * nt, [opposite], range(4), lambda _, t: place(t), far_v.at[parts + s], f_sem)
    for s in range(2 * parts):
        size = (4 if s < parts else 3) * seg
        landed(t_v.at[s, pl.ds(0, size), :], t_sem.at[s])
        spans = ((8 * seg, 0, 4 * seg),) if s < parts else ((0, 0, 2 * seg), (11 * seg, 2 * seg, seg))
        multiply(a_v, t_v.at[s], acc, s * nt, spans, True)
    landed(far_v, f_sem)


def far_multiply(low, mt, a_v, tile, acc, p_v, s):
    rows, nt = a_v.shape[0], tile.shape[1]

    @pl.loop(0, rows // mt)
    def _(t):
        at = pl.ds(pl.multiple_of(t * mt, mt), mt)
        to, cols = pl.ds(pl.multiple_of(low + t * mt, 128), mt), pl.ds(s * nt, nt)
        r = acc[to, cols] + jnp.dot(a_v[at, :], tile[...], preferred_element_type=jnp.float32)
        acc[to, cols] = r
        lanes = r[:, 0:128] * r[:, 0:128]
        for n in range(128, nt, 128):
            lanes = lanes + r[:, n:n + 128] * r[:, n:n + 128]
        p_v[at, :] = lanes if s == 0 else p_v[at, :] + lanes


def far_kernel(low, before, t_in, *refs):
    acc, t_v, power, a_v, p_v, a_sem = refs[-6:]
    chunks = refs[:-6] if low == 0 else refs[1:-6]
    at = 0
    for chunk in chunks:
        pltpu.make_async_copy(chunk, a_v.at[pl.ds(at, chunk.shape[0]), :], a_sem).start()
        at += chunk.shape[0]
    if low > 0:
        power[:, 0:low] = refs[0][...]
    landed(a_v, a_sem)
    for s in range(t_v.shape[0]):
        far_multiply(low, min(256, a_v.shape[0]), a_v, t_in.at[s], acc, p_v, s)
    for m in range(0, p_v.shape[0], 128):
        power[:, low + m:low + m + 128] = (
            jnp.sum(p_v[m:m + 128, :].T, axis=0, keepdims=True) + jnp.zeros((8, 128), jnp.float32))


def scale_kernel(cols, acc, *refs):
    powers, (out, o_v, o_sem) = refs[:4], refs[4:]
    blocks, size, _ = o_v.shape
    for i in range(blocks):
        lanes = pl.ds(i * size, size)
        total = (powers[0][0:1, lanes] + powers[1][0:1, lanes]) + (powers[2][0:1, lanes] + powers[3][0:1, lanes])
        factor = jnp.broadcast_to(lax.rsqrt(total / cols + 1e-06), (size, size)).T[:, 0:1]
        o_v[i] = acc[pl.ds(i * size, size), :] * factor
        pltpu.make_async_copy(o_v.at[i], out.at[pl.ds(i * size, size), :], o_sem.at[i]).start()
    for i in range(blocks):
        landed(o_v.at[i], o_sem.at[i])


ANY = pl.BlockSpec(memory_space=pltpu.HBM)
SMEM = pl.BlockSpec(memory_space=pltpu.SMEM)


VMEM = pl.BlockSpec(memory_space=pltpu.VMEM)


def kept(value):
    return pltpu.with_memory_space_constraint(value, pltpu.VMEM)


def apart(value):
    return pltpu.with_memory_space_constraint(value, pltpu.HBM)


def call(kernel, out_shape, in_specs, out_specs, scratch, flops, limit, aliases={}):
    return pl.pallas_call(
        kernel,
        out_shape=out_shape,
        in_specs=in_specs,
        out_specs=out_specs,
        scratch_shapes=scratch,
        input_output_aliases=aliases,
        cost_estimate=pl.CostEstimate(flops=flops, bytes_accessed=16 << 20, transcendentals=0),
        compiler_params=pltpu.CompilerParams(vmem_limit_bytes=limit << 20),
    )


def near(pos, left, behind, ahead, pieces):
    rows, depth = left.shape
    half, seg, low = pieces[0].shape[1], depth // 4, ahead[0].shape[0]
    total, gathered = pltpu.VMEM((rows, 2 * half), jnp.float32), pltpu.VMEM((rows, 12 * seg), left.dtype)
    both = total, gathered
    flops = 2 * rows * half * seg
    dma = pltpu.SemaphoreType.DMA
    tile = pltpu.VMEM((2, 8 * seg, NT), left.dtype)
    acc, blocks = call(
        functools.partial(left_kernel, low), both, [SMEM] + [ANY] * 10, (VMEM, VMEM),
        [tile, dma((2,)), dma((2, 2))], 6 * flops, NEAR_MIB,
    )(pos, left, *behind[:2], ahead[0], *pieces[:6])
    acc, blocks = call(
        functools.partial(right_kernel, low), both, [SMEM, VMEM, VMEM] + [ANY] * 12, (VMEM, VMEM),
        [pltpu.VMEM((2, 9 * seg, NT), left.dtype), dma((2,)), dma((2, 3))], 9 * flops, NEAR_MIB, {1: 1, 2: 0},
    )(pos, kept(blocks), kept(acc), left, *behind, *ahead, *pieces[8:14])
    acc, blocks = call(
        functools.partial(tail_kernel, low), both, [SMEM, VMEM, VMEM] + [ANY] * 6, (VMEM, VMEM),
        [tile, dma((2, 2))], 2 * flops, NEAR_MIB, {1: 1, 2: 0},
    )(pos, kept(blocks), kept(acc), *pieces[:6])
    parts = 2 * half // NT
    return call(
        rest_kernel, (total, pltpu.VMEM((parts, depth, NT), left.dtype)), [SMEM, VMEM, VMEM] + [ANY] * 16, (VMEM, VMEM),
        [pltpu.VMEM((parts, depth, NT), left.dtype), dma((parts,)), dma], 7 * flops, NEAR_MIB, {2: 0},
    )(pos, kept(blocks), kept(acc), *pieces)


def far(acc, tile, chunks, powers):
    depth = chunks[0].shape[1]
    rows = sum(chunk.shape[0] for chunk in chunks)
    low = powers[0].shape[1] if powers else 0
    out = pltpu.VMEM(acc.shape, acc.dtype), pltpu.VMEM(tile.shape, tile.dtype), jax.ShapeDtypeStruct((8, low + rows), jnp.float32)
    return call(
        functools.partial(far_kernel, low), out, [VMEM, VMEM] + [VMEM] * len(powers) + [ANY] * len(chunks), (VMEM, VMEM, VMEM),
        [pltpu.VMEM((rows, depth), chunks[0].dtype), pltpu.VMEM((rows, 128), jnp.float32), pltpu.SemaphoreType.DMA],
        2 * rows * depth * acc.shape[1], FAR_MIB, {0: 0, 1: 1},
    )(kept(acc), kept(tile), *powers, *chunks)


def scale(cols, acc, powers):
    rows, width = acc.shape
    return call(
        functools.partial(scale_kernel, cols), jax.ShapeDtypeStruct(acc.shape, jnp.float32), [VMEM] * 5, ANY,
        [pltpu.VMEM((rows // 128, 128, width), jnp.float32), pltpu.SemaphoreType.DMA((rows // 128,))],
        rows * width * 30, 12,
    )(kept(acc), *powers)


def per_device(left, right):
    width = right.shape[1]
    half = width // 2
    me, z = lax.axis_index("gy"), lax.axis_index("gx")
    pos = jnp.stack([me // (NX * NC), (me // NC) % NX, me % NC, z]).astype(jnp.int32)

    most = sum(ROW_CHUNKS[:-1])
    ahead = [move(left[:most], "z", False), move(left[most:], "z", False)]
    behind, opposite, low = [], [], 0
    for i, size in enumerate(ROW_CHUNKS):
        behind.append(move(left[low:low + size], "z", True))
        opposite.append(move(behind[i], "z", True))
        low += size
    pieces = []
    for h, (a, b) in enumerate((("x", "y"), ("y", "x"))):
        line = jnp.concatenate(ring(right[:, h * half:(h + 1) * half], a), axis=0)
        for v in ring(line, b):
            pieces += [v, move(v, "core", True)]

    pieces = [apart(v) for v in pieces]
    acc, tile = near(pos, apart(left), [apart(v) for v in behind], [apart(v) for v in ahead], pieces)
    acc, tile, power = far(acc, tile, opposite[:-1], [])
    acc, tile, power = far(acc, tile, opposite[-1:], [power])
    return scale(width * NZ, acc, exchange(power))


def solution(mesh):
    placed = (P("gy", "gx"), P("gy", "gx"))
    return jax.shard_map(per_device, mesh=mesh, in_specs=placed, out_specs=P("gy", "gx"), check_vma=False)
```

```python
import functools

import jax
import jax.numpy as jnp
from jax import lax
from jax.experimental import pallas as pl
from jax.experimental.pallas import tpu as pltpu
from jax.sharding import PartitionSpec as P


ROW_CHUNKS = (384, 384, 256)
NX = NY = NZ = 4
NC = 2
NT = 512

NEAR_MIB, FAR_MIB = 11, 6


def gy(y, x, c):
    return ((y % NY) * NX + x % NX) * NC + c


def along(axis, first):
    pairs = []
    for y in range(NY):
        for x in range(NX):
            for c in range(NC):
                step = 1 if (c == 0) == first else -1
                if axis == "x":
                    pairs.append((gy(y, x, c), gy(y, x + step, c)))
                elif axis == "y":
                    pairs.append((gy(y, x, c), gy(y + step, x, c)))
                elif axis == "core":
                    pairs.append((gy(y, x, c), gy(y, x, 1 - c)))
                else:
                    for z in range(NZ):
                        pairs.append((gy(y, x, c) * NZ + z, gy(y, x, c) * NZ + (z + step) % NZ))
    return pairs


def move(value, axis, first):
    name = ("gy", "gx") if axis == "z" else "gy"
    return lax.ppermute(value, name, along(axis, first))


def ring(value, axis):
    behind = move(value, axis, True)
    ahead = move(value, axis, False)
    return [value, behind, ahead, move(behind, axis, True)]


def exchange(power):
    opposite = lax.ppermute(power, "gx", [(i, (i + 2) % NZ) for i in range(NZ)])
    return [power, move(power, "z", True), move(power, "z", False), opposite]


def offset(slot, core):
    back = jnp.where(core == 0, 3, 1)
    return (0, back, 4 - back, 2)[slot]


def slot_of(distance, core):
    near = jnp.where((distance == 3) == (core == 0), 1, 2)
    return jnp.where(distance == 0, 0, jnp.where(distance == 2, 3, near))


def plan(pos):
    y0, core, z0 = pos[0], pos[2], pos[3]
    d = lax.rem(z0 - y0 + 4, 4)
    order = (
        jnp.where((d == 1) | (d == 2), 3, 0),
        jnp.where(d == 1, 0, 1),
        jnp.where(d == 2, 0, jnp.where(d == 1, 1, 3)),
    )
    where = []
    for b in range(3):
        distance = offset(b, core)
        where.append(jnp.where(distance == order[0], 0, jnp.where(distance == order[1], 1, 2)))
    return [lax.rem(z0 + o, 4) for o in order], where


def turned(x, x0):
    return lax.rem(x - x0 + 5, 4)


def copy_left_half(pos, pieces, n, y, lines, place, tile, sem):
    step = pieces[0][0][0].shape[0] // 4
    for q in range(2):
        core = pos[2] if q == 0 else 1 - pos[2]
        line = slot_of(lax.rem(y - pos[0] + 4, 4), core)
        to = [pl.multiple_of(place(lax.rem(offset(r, core) + 1, 4)) + core * step, step) for r in range(4)]
        for k in lines:
            @pl.when(line == k)
            def _():
                for r in range(4):
                    src = pieces[0][k][q].at[pl.ds(r * step, step), pl.ds(n, tile.shape[1])]
                    pltpu.make_async_copy(src, tile.at[pl.ds(to[r], step), :], sem).start()


def copy_right_half(pos, pieces, n, ys, lines, place, tile, sem):
    step = pieces[1][lines[0]][0].shape[0] // 4
    for q in range(2):
        core = pos[2] if q == 0 else 1 - pos[2]
        at = [pl.multiple_of(slot_of(lax.rem(y - pos[0] + 4, 4), core) * step, step) for y in ys]
        for k in lines:
            turn = lax.rem(offset(k, core) + 1, 4)
            for p in range(len(ys)):
                to = pl.multiple_of(place(p, turn) + core * step, step)
                src = pieces[1][k][q].at[pl.ds(at[p], step), pl.ds(n, tile.shape[1])]
                pltpu.make_async_copy(src, tile.at[pl.ds(to, step), :], sem).start()


def copy_left(chunks, low, place, seg, dst, sem):
    for chunk in chunks:
        rows = pl.ds(low, chunk.shape[0])
        for x in range(4):
            col = pl.ds(pl.multiple_of(place(x), seg), seg)
            pltpu.make_async_copy(chunk.at[:, pl.ds(x * seg, seg)], dst.at[rows, col], sem).start()
        low += chunk.shape[0]


def landed(ref, sem):
    pltpu.make_async_copy(ref, ref, sem).wait()


def nest(flat):
    return [[[flat[(h * 4 + line) * 2 + q] for q in range(2)] for line in range(4)] for h in range(2)]


def spot(p, t, seg):
    return jnp.where(t == 3, jnp.where(p == 2, 11, p), 2 + 3 * p + t) * seg


def multiply(a_v, tile, acc, col, spans, add, low=0, high=None):
    rows, nt = (high or a_v.shape[0]) - low, tile.shape[1]
    mt = max(m for m in (512, 384, 256) if rows % m == 0)

    @pl.loop(0, rows // mt)
    def _(t):
        at = pl.ds(pl.multiple_of(low + t * mt, 128), mt)
        cols = pl.ds(col, nt)
        r = acc[at, cols] if add else None
        for a, b, size in spans:
            d = jnp.dot(a_v[at, pl.ds(a, size)], tile[pl.ds(b, size), :], preferred_element_type=jnp.float32)
            r = d if r is None else r + d
        acc[at, cols] = r


def left_tiles(pos, lines, blocks, nt, seg, t_v, t_sem):
    pieces = [[lines[2 * k:2 * k + 2] for k in range(3)]]

    def fetch(s, p):
        copy_left_half(
            pos, pieces, s * nt, blocks[p], range(3), lambda t: spot(p, t, seg), t_v.at[s % 2], t_sem.at[s % 2, p])

    return fetch


def left_kernel(low, pos, left, *refs):
    (first, second, side), lines, (acc, a_v, t_v, a_sem, t_sem) = refs[:3], refs[3:9], refs[9:]
    sources = [left.at[pl.ds(0, low), :]], [first, second], [side.at[pl.ds(0, low), :]]
    half, nt, seg = acc.shape[1] // 2, t_v.shape[2], a_v.shape[1] // 12
    blocks, where = plan(pos)
    fetch = left_tiles(pos, lines, blocks, nt, seg, t_v, t_sem)
    for p in range(2):
        for b in range(3):
            @pl.when(where[b] == p)
            def _():
                copy_left(sources[b], 0, lambda x: spot(p, turned(x, pos[1]), seg), seg, a_v, a_sem.at[p])
        fetch(0, p)
    for s in range(half // nt):
        for p in range(2):
            if (s + 1) * nt < half:
                fetch(s + 1, p)
        for p in range(2):
            if s == 0:
                landed(a_v.at[pl.ds(0, low), pl.ds(0, 4 * seg)], a_sem.at[p])
            landed(t_v.at[s % 2, pl.ds(0, 4 * seg), :], t_sem.at[s % 2, p])
            if s == 0:
                one, three = p * seg, (2 + 3 * p) * seg
                multiply(a_v, t_v.at[0], acc, 0, ((one, one, seg), (three, three, 3 * seg)), p > 0, 0, low)
        if s > 0:
            multiply(a_v, t_v.at[s % 2], acc, s * nt, ((0, 0, 8 * seg),), False, 0, low)


def right_kernel(low, pos, a_in, before, left, *refs):
    chunks, side, lines, (acc, a_v, t_v, a_sem, t_sem) = refs[:3], refs[3], refs[4:10], refs[10:]
    rows = left.shape[0]
    upper = [left.at[pl.ds(0, low), :]], chunks[:2], [side.at[pl.ds(0, low), :]]
    lower = [left.at[pl.ds(low, rows - low), :]], chunks[2:], [side.at[pl.ds(low, rows - low), :]]
    pieces = [None, [lines[2 * k:2 * k + 2] for k in range(3)]]
    half, nt, seg = acc.shape[1] // 2, t_v.shape[2], a_v.shape[1] // 12
    blocks, where = plan(pos)

    def fetch(s, p):
        copy_right_half(
            pos, pieces, s * nt, [blocks[p]], range(3), lambda _, t: (3 * p + t) * seg, t_v.at[s % 2], t_sem.at[s % 2, p])

    for p in range(3):
        fetch(0, p)
    for b in range(3):
        @pl.when(where[b] == 2)
        def _():
            copy_left(upper[b], 0, lambda x: spot(2, turned(x, pos[1]), seg), seg, a_v, a_sem.at[1])
    for b in range(3):
        copy_left(lower[b], low, lambda x: spot(where[b], turned(x, pos[1]), seg), seg, a_v, a_sem.at[0])
    for s in range(half // nt):
        for p in range(3):
            if (s + 1) * nt < half:
                fetch(s + 1, p)
        for p in range(3):
            if (s, p) == (0, 2):
                landed(a_v.at[pl.ds(0, low), pl.ds(0, 4 * seg)], a_sem.at[1])
            landed(t_v.at[s % 2, pl.ds(0, 3 * seg), :], t_sem.at[s % 2, p])
            if s == 0:
                multiply(a_v, t_v.at[0], acc, half, (((2 + 3 * p) * seg, 3 * p * seg, 3 * seg),), p > 0, 0, low)
        if s == 0:
            landed(a_v.at[pl.ds(low, rows - low), :], a_sem.at[0])
        multiply(a_v, t_v.at[s % 2], acc, half + s * nt, ((2 * seg, 0, 9 * seg),), False, low if s == 0 else 0)


def tail_kernel(low, pos, a_in, before, *refs):
    lines, (acc, a_v, t_v, t_sem) = refs[:6], refs[6:]
    half, nt, seg = acc.shape[1] // 2, t_v.shape[2], a_v.shape[1] // 12
    blocks, _ = plan(pos)
    fetch = left_tiles(pos, lines, blocks, nt, seg, t_v, t_sem)
    for s in range(half // nt):
        for p in range(2):
            fetch(s, p)
    for s in range(half // nt):
        for p in range(2):
            landed(t_v.at[s, pl.ds(0, 4 * seg), :], t_sem.at[s, p])
            one, three = p * seg, (2 + 3 * p) * seg
            multiply(a_v, t_v.at[s], acc, s * nt, ((one, one, seg), (three, three, 3 * seg)), p > 0, low)


def rest_kernel(pos, a_v, before, *refs):
    pieces, (acc, far_v, t_v, t_sem, f_sem) = nest(refs[:16]), refs[16:]
    half, nt, seg = acc.shape[1] // 2, t_v.shape[2], a_v.shape[1] // 12
    blocks, _ = plan(pos)
    parts = half // nt
    for s in range(parts):
        copy_left_half(pos, pieces, s * nt, blocks[2], range(4), lambda t: t * seg, t_v.at[s], t_sem.at[s])
    for s in range(parts):
        copy_right_half(
            pos, pieces, s * nt, blocks, (3,), lambda p, t: p * seg, t_v.at[parts + s], t_sem.at[parts + s])

    def place(t):
        return lax.rem(pos[1] + t + 3, 4) * seg

    opposite = lax.rem(pos[3] + 2, 4)
    for s in range(parts):
        copy_left_half(pos, pieces, s * nt, opposite, range(4), place, far_v.at[s], f_sem)
        copy_right_half(
            pos, pieces, s * nt, [opposite], range(4), lambda _, t: place(t), far_v.at[parts + s], f_sem)
    for s in range(2 * parts):
        size = (4 if s < parts else 3) * seg
        landed(t_v.at[s, pl.ds(0, size), :], t_sem.at[s])
        spans = ((8 * seg, 0, 4 * seg),) if s < parts else ((0, 0, 2 * seg), (11 * seg, 2 * seg, seg))
        multiply(a_v, t_v.at[s], acc, s * nt, spans, True)
    landed(far_v, f_sem)


def far_multiply(low, mt, a_v, tile, acc, p_v, s):
    rows, nt = a_v.shape[0], tile.shape[1]

    @pl.loop(0, rows // mt)
    def _(t):
        at = pl.ds(pl.multiple_of(t * mt, mt), mt)
        to, cols = pl.ds(pl.multiple_of(low + t * mt, 128), mt), pl.ds(s * nt, nt)
        r = acc[to, cols] + jnp.dot(a_v[at, :], tile[...], preferred_element_type=jnp.float32)
        acc[to, cols] = r
        lanes = r[:, 0:128] * r[:, 0:128]
        for n in range(128, nt, 128):
            lanes = lanes + r[:, n:n + 128] * r[:, n:n + 128]
        p_v[at, :] = lanes if s == 0 else p_v[at, :] + lanes


def far_kernel(low, before, t_in, *refs):
    acc, t_v, power, a_v, p_v, a_sem = refs[-6:]
    chunks = refs[:-6] if low == 0 else refs[1:-6]
    at = 0
    for chunk in chunks:
        pltpu.make_async_copy(chunk, a_v.at[pl.ds(at, chunk.shape[0]), :], a_sem).start()
        at += chunk.shape[0]
    if low > 0:
        power[:, 0:low] = refs[0][...]
    landed(a_v, a_sem)
    for s in range(t_v.shape[0]):
        far_multiply(low, min(256, a_v.shape[0]), a_v, t_in.at[s], acc, p_v, s)
    for m in range(0, p_v.shape[0], 128):
        power[:, low + m:low + m + 128] = (
            jnp.sum(p_v[m:m + 128, :].T, axis=0, keepdims=True) + jnp.zeros((8, 128), jnp.float32))


def scale_kernel(cols, acc, *refs):
    powers, (out, o_v, o_sem) = refs[:4], refs[4:]
    blocks, size, _ = o_v.shape
    for i in range(blocks):
        lanes = pl.ds(i * size, size)
        total = (powers[0][0:1, lanes] + powers[1][0:1, lanes]) + (powers[2][0:1, lanes] + powers[3][0:1, lanes])
        factor = jnp.broadcast_to(lax.rsqrt(total / cols + 1e-06), (size, size)).T[:, 0:1]
        o_v[i] = acc[pl.ds(i * size, size), :] * factor
        pltpu.make_async_copy(o_v.at[i], out.at[pl.ds(i * size, size), :], o_sem.at[i]).start()
    for i in range(blocks):
        landed(o_v.at[i], o_sem.at[i])


ANY = pl.BlockSpec(memory_space=pltpu.HBM)
SMEM = pl.BlockSpec(memory_space=pltpu.SMEM)


VMEM = pl.BlockSpec(memory_space=pltpu.VMEM)


def kept(value):
    return pltpu.with_memory_space_constraint(value, pltpu.VMEM)


def apart(value):
    return pltpu.with_memory_space_constraint(value, pltpu.HBM)


def call(kernel, out_shape, in_specs, out_specs, scratch, flops, limit, aliases={}):
    return pl.pallas_call(
        kernel,
        out_shape=out_shape,
        in_specs=in_specs,
        out_specs=out_specs,
        scratch_shapes=scratch,
        input_output_aliases=aliases,
        cost_estimate=pl.CostEstimate(flops=flops, bytes_accessed=16 << 20, transcendentals=0),
        compiler_params=pltpu.CompilerParams(vmem_limit_bytes=limit << 20),
    )


def near(pos, left, behind, ahead, pieces):
    rows, depth = left.shape
    half, seg, low = pieces[0].shape[1], depth // 4, rows - behind[-1].shape[0]
    total, gathered = pltpu.VMEM((rows, 2 * half), jnp.float32), pltpu.VMEM((rows, 12 * seg), left.dtype)
    both = total, gathered
    flops = 2 * rows * half * seg
    dma = pltpu.SemaphoreType.DMA
    tile = pltpu.VMEM((2, 8 * seg, NT), left.dtype)
    acc, blocks = call(
        functools.partial(left_kernel, low), both, [SMEM] + [ANY] * 10, (VMEM, VMEM),
        [tile, dma((2,)), dma((2, 2))], 6 * flops, NEAR_MIB,
    )(pos, left, *behind[:2], ahead, *pieces[:6])
    acc, blocks = call(
        functools.partial(right_kernel, low), both, [SMEM, VMEM, VMEM] + [ANY] * 11, (VMEM, VMEM),
        [pltpu.VMEM((2, 9 * seg, NT), left.dtype), dma((2,)), dma((2, 3))], 9 * flops, NEAR_MIB, {1: 1, 2: 0},
    )(pos, kept(blocks), kept(acc), left, *behind, ahead, *pieces[8:14])
    acc, blocks = call(
        functools.partial(tail_kernel, low), both, [SMEM, VMEM, VMEM] + [ANY] * 6, (VMEM, VMEM),
        [tile, dma((2, 2))], 2 * flops, NEAR_MIB, {1: 1, 2: 0},
    )(pos, kept(blocks), kept(acc), *pieces[:6])
    parts = 2 * half // NT
    return call(
        rest_kernel, (total, pltpu.VMEM((parts, depth, NT), left.dtype)), [SMEM, VMEM, VMEM] + [ANY] * 16, (VMEM, VMEM),
        [pltpu.VMEM((parts, depth, NT), left.dtype), dma((parts,)), dma], 7 * flops, NEAR_MIB, {2: 0},
    )(pos, kept(blocks), kept(acc), *pieces)


def far(acc, tile, chunks, powers):
    depth = chunks[0].shape[1]
    rows = sum(chunk.shape[0] for chunk in chunks)
    low = powers[0].shape[1] if powers else 0
    out = pltpu.VMEM(acc.shape, acc.dtype), pltpu.VMEM(tile.shape, tile.dtype), jax.ShapeDtypeStruct((8, low + rows), jnp.float32)
    return call(
        functools.partial(far_kernel, low), out, [VMEM, VMEM] + [VMEM] * len(powers) + [ANY] * len(chunks), (VMEM, VMEM, VMEM),
        [pltpu.VMEM((rows, depth), chunks[0].dtype), pltpu.VMEM((rows, 128), jnp.float32), pltpu.SemaphoreType.DMA],
        2 * rows * depth * acc.shape[1], FAR_MIB, {0: 0, 1: 1},
    )(kept(acc), kept(tile), *powers, *chunks)


def scale(cols, acc, powers):
    rows, width = acc.shape
    return call(
        functools.partial(scale_kernel, cols), jax.ShapeDtypeStruct(acc.shape, jnp.float32), [VMEM] * 5, ANY,
        [pltpu.VMEM((rows // 128, 128, width), jnp.float32), pltpu.SemaphoreType.DMA((rows // 128,))],
        rows * width * 30, 12,
    )(kept(acc), *powers)


def per_device(left, right):
    width = right.shape[1]
    half = width // 2
    me, z = lax.axis_index("gy"), lax.axis_index("gx")
    pos = jnp.stack([me // (NX * NC), (me // NC) % NX, me % NC, z]).astype(jnp.int32)

    ahead = move(left, "z", False)
    behind, opposite, low = [], [], 0
    for i, size in enumerate(ROW_CHUNKS):
        behind.append(move(left[low:low + size], "z", True))
        opposite.append(move(behind[i], "z", True))
        low += size
    pieces = []
    for h, (a, b) in enumerate((("x", "y"), ("y", "x"))):
        line = jnp.concatenate(ring(right[:, h * half:(h + 1) * half], a), axis=0)
        for v in ring(line, b):
            pieces += [v, move(v, "core", True)]

    pieces = [v if i % 8 == 7 else apart(v) for i, v in enumerate(pieces)]
    acc, tile = near(pos, apart(left), [apart(v) for v in behind], apart(ahead), pieces)
    acc, tile, power = far(acc, tile, opposite[:-1], [])
    acc, tile, power = far(acc, tile, opposite[-1:], [power])
    return scale(width * NZ, acc, exchange(power))


def solution(mesh):
    placed = (P("gy", "gx"), P("gy", "gx"))
    return jax.shard_map(per_device, mesh=mesh, in_specs=placed, out_specs=P("gy", "gx"), check_vma=False)
```

```python
import functools

import jax
import jax.numpy as jnp
from jax import lax
from jax.experimental import pallas as pl
from jax.experimental.pallas import tpu as pltpu
from jax.sharding import PartitionSpec as P


ROW_CHUNKS = (384, 384, 256)
NX = NY = NZ = 4
NC = 2
NT = 512

NEAR_MIB, FAR_MIB = 11, 6


def gy(y, x, c):
    return ((y % NY) * NX + x % NX) * NC + c


def along(axis, first):
    pairs = []
    for y in range(NY):
        for x in range(NX):
            for c in range(NC):
                step = 1 if (c == 0) == first else -1
                if axis == "x":
                    pairs.append((gy(y, x, c), gy(y, x + step, c)))
                elif axis == "y":
                    pairs.append((gy(y, x, c), gy(y + step, x, c)))
                elif axis == "core":
                    pairs.append((gy(y, x, c), gy(y, x, 1 - c)))
                else:
                    for z in range(NZ):
                        pairs.append((gy(y, x, c) * NZ + z, gy(y, x, c) * NZ + (z + step) % NZ))
    return pairs


def move(value, axis, first):
    name = ("gy", "gx") if axis == "z" else "gy"
    return lax.ppermute(value, name, along(axis, first))


def ring(value, axis):
    behind = move(value, axis, True)
    ahead = move(value, axis, False)
    return [value, behind, ahead, move(behind, axis, True)]


def exchange(power):
    opposite = lax.ppermute(power, "gx", [(i, (i + 2) % NZ) for i in range(NZ)])
    return [power, move(power, "z", True), move(power, "z", False), opposite]


def offset(slot, core):
    back = jnp.where(core == 0, 3, 1)
    return (0, back, 4 - back, 2)[slot]


def slot_of(distance, core):
    near = jnp.where((distance == 3) == (core == 0), 1, 2)
    return jnp.where(distance == 0, 0, jnp.where(distance == 2, 3, near))


def plan(pos):
    y0, core, z0 = pos[0], pos[2], pos[3]
    d = lax.rem(z0 - y0 + 4, 4)
    order = (
        jnp.where((d == 1) | (d == 2), 3, 0),
        jnp.where(d == 1, 0, 1),
        jnp.where(d == 2, 0, jnp.where(d == 1, 1, 3)),
    )
    where = []
    for b in range(3):
        distance = offset(b, core)
        where.append(jnp.where(distance == order[0], 0, jnp.where(distance == order[1], 1, 2)))
    return [lax.rem(z0 + o, 4) for o in order], where


def turned(x, x0):
    return lax.rem(x - x0 + 5, 4)


def copy_left_half(pos, pieces, n, y, lines, place, tile, sem):
    step = pieces[0][0][0].shape[0] // 4
    for q in range(2):
        core = pos[2] if q == 0 else 1 - pos[2]
        line = slot_of(lax.rem(y - pos[0] + 4, 4), core)
        to = [pl.multiple_of(place(lax.rem(offset(r, core) + 1, 4)) + core * step, step) for r in range(4)]
        for k in lines:
            @pl.when(line == k)
            def _():
                for r in range(4):
                    src = pieces[0][k][q].at[pl.ds(r * step, step), pl.ds(n, tile.shape[1])]
                    pltpu.make_async_copy(src, tile.at[pl.ds(to[r], step), :], sem).start()


def copy_right_half(pos, pieces, n, ys, lines, place, tile, sem):
    step = pieces[1][lines[0]][0].shape[0] // 4
    for q in range(2):
        core = pos[2] if q == 0 else 1 - pos[2]
        at = [pl.multiple_of(slot_of(lax.rem(y - pos[0] + 4, 4), core) * step, step) for y in ys]
        for k in lines:
            turn = lax.rem(offset(k, core) + 1, 4)
            for p in range(len(ys)):
                to = pl.multiple_of(place(p, turn) + core * step, step)
                src = pieces[1][k][q].at[pl.ds(at[p], step), pl.ds(n, tile.shape[1])]
                pltpu.make_async_copy(src, tile.at[pl.ds(to, step), :], sem).start()


def copy_left(chunks, low, place, seg, dst, sem):
    for chunk in chunks:
        rows = pl.ds(low, chunk.shape[0])
        for x in range(4):
            col = pl.ds(pl.multiple_of(place(x), seg), seg)
            pltpu.make_async_copy(chunk.at[:, pl.ds(x * seg, seg)], dst.at[rows, col], sem).start()
        low += chunk.shape[0]


def landed(ref, sem):
    pltpu.make_async_copy(ref, ref, sem).wait()


def nest(flat):
    return [[[flat[(h * 4 + line) * 2 + q] for q in range(2)] for line in range(4)] for h in range(2)]


def spot(p, t, seg):
    return jnp.where(t == 3, jnp.where(p == 2, 11, p), 2 + 3 * p + t) * seg


def multiply(a_v, tile, acc, col, spans, add, low=0, high=None):
    rows, nt = (high or a_v.shape[0]) - low, tile.shape[1]
    mt = max(m for m in (512, 384, 256) if rows % m == 0)

    @pl.loop(0, rows // mt)
    def _(t):
        at = pl.ds(pl.multiple_of(low + t * mt, 128), mt)
        cols = pl.ds(col, nt)
        r = acc[at, cols] if add else None
        for a, b, size in spans:
            d = jnp.dot(a_v[at, pl.ds(a, size)], tile[pl.ds(b, size), :], preferred_element_type=jnp.float32)
            r = d if r is None else r + d
        acc[at, cols] = r


def left_tiles(pos, lines, blocks, nt, seg, t_v, t_sem):
    pieces = [[lines[2 * k:2 * k + 2] for k in range(3)]]

    def fetch(s, p):
        copy_left_half(
            pos, pieces, s * nt, blocks[p], range(3), lambda t: spot(p, t, seg), t_v.at[s % 2], t_sem.at[s % 2, p])

    return fetch


def left_kernel(low, pos, left, *refs):
    (first, second, side), lines, (acc, a_v, t_v, a_sem, t_sem) = refs[:3], refs[3:9], refs[9:]
    sources = [left.at[pl.ds(0, low), :]], [first, second], [side.at[pl.ds(0, low), :]]
    half, nt, seg = acc.shape[1] // 2, t_v.shape[2], a_v.shape[1] // 12
    blocks, where = plan(pos)
    fetch = left_tiles(pos, lines, blocks, nt, seg, t_v, t_sem)
    for p in range(2):
        for b in range(3):
            @pl.when(where[b] == p)
            def _():
                copy_left(sources[b], 0, lambda x: spot(p, turned(x, pos[1]), seg), seg, a_v, a_sem.at[p])
        fetch(0, p)
    for s in range(half // nt):
        for p in range(2):
            if s == 0:
                landed(a_v.at[pl.ds(0, low), pl.ds(0, 4 * seg)], a_sem.at[p])
            landed(t_v.at[s % 2, pl.ds(0, 4 * seg), :], t_sem.at[s % 2, p])
            if s == 0:
                one, three = p * seg, (2 + 3 * p) * seg
                multiply(a_v, t_v.at[0], acc, 0, ((one, one, seg), (three, three, 3 * seg)), p > 0, 0, low)
            if p == 0 and (s + 1) * nt < half:
                fetch(s + 1, 0)
                fetch(s + 1, 1)
        if s > 0:
            multiply(a_v, t_v.at[s % 2], acc, s * nt, ((0, 0, 8 * seg),), False, 0, low)


def right_kernel(low, pos, a_in, before, left, *refs):
    chunks, side, lines, (acc, a_v, t_v, a_sem, t_sem) = refs[:3], refs[3], refs[4:10], refs[10:]
    rows = left.shape[0]
    upper = [left.at[pl.ds(0, low), :]], chunks[:2], [side.at[pl.ds(0, low), :]]
    lower = [left.at[pl.ds(low, rows - low), :]], chunks[2:], [side.at[pl.ds(low, rows - low), :]]
    pieces = [None, [lines[2 * k:2 * k + 2] for k in range(3)]]
    half, nt, seg = acc.shape[1] // 2, t_v.shape[2], a_v.shape[1] // 12
    blocks, where = plan(pos)

    def fetch(s, p):
        copy_right_half(
            pos, pieces, s * nt, [blocks[p]], range(3), lambda _, t: (3 * p + t) * seg, t_v.at[s % 2], t_sem.at[s % 2, p])

    for p in range(3):
        fetch(0, p)
    for b in range(3):
        @pl.when(where[b] == 2)
        def _():
            copy_left(upper[b], 0, lambda x: spot(2, turned(x, pos[1]), seg), seg, a_v, a_sem.at[1])
    for b in range(3):
        copy_left(lower[b], low, lambda x: spot(where[b], turned(x, pos[1]), seg), seg, a_v, a_sem.at[0])
    for s in range(half // nt):
        for p in range(3):
            if (s + 1) * nt < half:
                fetch(s + 1, p)
        for p in range(3):
            if (s, p) == (0, 2):
                landed(a_v.at[pl.ds(0, low), pl.ds(0, 4 * seg)], a_sem.at[1])
            landed(t_v.at[s % 2, pl.ds(0, 3 * seg), :], t_sem.at[s % 2, p])
            if s == 0:
                multiply(a_v, t_v.at[0], acc, half, (((2 + 3 * p) * seg, 3 * p * seg, 3 * seg),), p > 0, 0, low)
        if s == 0:
            landed(a_v.at[pl.ds(low, rows - low), :], a_sem.at[0])
        multiply(a_v, t_v.at[s % 2], acc, half + s * nt, ((2 * seg, 0, 9 * seg),), False, low if s == 0 else 0)


def tail_kernel(low, pos, a_in, before, *refs):
    lines, (acc, a_v, t_v, t_sem) = refs[:6], refs[6:]
    half, nt, seg = acc.shape[1] // 2, t_v.shape[2], a_v.shape[1] // 12
    blocks, _ = plan(pos)
    fetch = left_tiles(pos, lines, blocks, nt, seg, t_v, t_sem)
    for s in range(half // nt):
        for p in range(2):
            fetch(s, p)
    for s in range(half // nt):
        for p in range(2):
            landed(t_v.at[s, pl.ds(0, 4 * seg), :], t_sem.at[s, p])
            one, three = p * seg, (2 + 3 * p) * seg
            multiply(a_v, t_v.at[s], acc, s * nt, ((one, one, seg), (three, three, 3 * seg)), p > 0, low)


def rest_kernel(pos, a_v, before, *refs):
    pieces, (acc, far_v, t_v, t_sem, f_sem) = nest(refs[:16]), refs[16:]
    half, nt, seg = acc.shape[1] // 2, t_v.shape[2], a_v.shape[1] // 12
    blocks, _ = plan(pos)
    parts = half // nt
    for s in range(parts):
        copy_left_half(pos, pieces, s * nt, blocks[2], range(4), lambda t: t * seg, t_v.at[s], t_sem.at[s])
    for s in range(parts):
        copy_right_half(
            pos, pieces, s * nt, blocks, (3,), lambda p, t: p * seg, t_v.at[parts + s], t_sem.at[parts + s])

    def place(t):
        return lax.rem(pos[1] + t + 3, 4) * seg

    opposite = lax.rem(pos[3] + 2, 4)
    for s in range(parts):
        copy_left_half(pos, pieces, s * nt, opposite, range(4), place, far_v.at[s], f_sem)
        copy_right_half(
            pos, pieces, s * nt, [opposite], range(4), lambda _, t: place(t), far_v.at[parts + s], f_sem)
    for s in range(2 * parts):
        size = (4 if s < parts else 3) * seg
        landed(t_v.at[s, pl.ds(0, size), :], t_sem.at[s])
        spans = ((8 * seg, 0, 4 * seg),) if s < parts else ((0, 0, 2 * seg), (11 * seg, 2 * seg, seg))
        multiply(a_v, t_v.at[s], acc, s * nt, spans, True)
    landed(far_v, f_sem)


def far_multiply(low, first, count, a_v, tile, acc, p_v, s):
    nt = tile.shape[1]
    mt = max(m for m in (384, 256) if count % m == 0)

    @pl.loop(0, count // mt)
    def _(t):
        at = pl.ds(pl.multiple_of(first + t * mt, 128), mt)
        to, cols = pl.ds(pl.multiple_of(low + first + t * mt, 128), mt), pl.ds(s * nt, nt)
        r = acc[to, cols] + jnp.dot(a_v[at, :], tile[...], preferred_element_type=jnp.float32)
        acc[to, cols] = r
        lanes = r[:, 0:128] * r[:, 0:128]
        for n in range(128, nt, 128):
            lanes = lanes + r[:, n:n + 128] * r[:, n:n + 128]
        p_v[at, :] = lanes if s == 0 else p_v[at, :] + lanes


def far_kernel(low, before, t_in, *refs):
    acc, t_v, power, a_v, p_v, a_sem = refs[-6:]
    chunks = refs[:-6] if low == 0 else refs[1:-6]
    sizes = [chunk.shape[0] for chunk in chunks]
    for i, chunk in enumerate(chunks):
        pltpu.make_async_copy(chunk, a_v.at[pl.ds(sum(sizes[:i]), sizes[i]), :], a_sem.at[i]).start()
    if low > 0:
        power[:, 0:low] = refs[0][...]
    for i, size in enumerate(sizes):
        landed(a_v.at[pl.ds(sum(sizes[:i]), size), :], a_sem.at[i])
        far_multiply(low, sum(sizes[:i]), size, a_v, t_in.at[0], acc, p_v, 0)
    for s in range(1, t_v.shape[0]):
        far_multiply(low, 0, sum(sizes), a_v, t_in.at[s], acc, p_v, s)
    for m in range(0, p_v.shape[0], 128):
        power[:, low + m:low + m + 128] = (
            jnp.sum(p_v[m:m + 128, :].T, axis=0, keepdims=True) + jnp.zeros((8, 128), jnp.float32))


def scale_kernel(cols, acc, *refs):
    powers, (out, o_v, o_sem) = refs[:4], refs[4:]
    blocks, size, _ = o_v.shape
    for i in range(blocks):
        lanes = pl.ds(i * size, size)
        total = (powers[0][0:1, lanes] + powers[1][0:1, lanes]) + (powers[2][0:1, lanes] + powers[3][0:1, lanes])
        factor = jnp.broadcast_to(lax.rsqrt(total / cols + 1e-06), (size, size)).T[:, 0:1]
        o_v[i] = acc[pl.ds(i * size, size), :] * factor
        pltpu.make_async_copy(o_v.at[i], out.at[pl.ds(i * size, size), :], o_sem.at[i]).start()
    for i in range(blocks):
        landed(o_v.at[i], o_sem.at[i])


ANY = pl.BlockSpec(memory_space=pltpu.HBM)
SMEM = pl.BlockSpec(memory_space=pltpu.SMEM)


VMEM = pl.BlockSpec(memory_space=pltpu.VMEM)


def kept(value):
    return pltpu.with_memory_space_constraint(value, pltpu.VMEM)


def apart(value):
    return pltpu.with_memory_space_constraint(value, pltpu.HBM)


def call(kernel, out_shape, in_specs, out_specs, scratch, flops, limit, aliases={}):
    return pl.pallas_call(
        kernel,
        out_shape=out_shape,
        in_specs=in_specs,
        out_specs=out_specs,
        scratch_shapes=scratch,
        input_output_aliases=aliases,
        cost_estimate=pl.CostEstimate(flops=flops, bytes_accessed=16 << 20, transcendentals=0),
        compiler_params=pltpu.CompilerParams(vmem_limit_bytes=limit << 20),
    )


def near(pos, left, behind, ahead, pieces):
    rows, depth = left.shape
    half, seg, low = pieces[0].shape[1], depth // 4, rows - behind[-1].shape[0]
    total, gathered = pltpu.VMEM((rows, 2 * half), jnp.float32), pltpu.VMEM((rows, 12 * seg), left.dtype)
    both = total, gathered
    flops = 2 * rows * half * seg
    dma = pltpu.SemaphoreType.DMA
    tile = pltpu.VMEM((2, 8 * seg, NT), left.dtype)
    acc, blocks = call(
        functools.partial(left_kernel, low), both, [SMEM] + [ANY] * 10, (VMEM, VMEM),
        [tile, dma((2,)), dma((2, 2))], 6 * flops, NEAR_MIB,
    )(pos, left, *behind[:2], ahead, *pieces[:6])
    acc, blocks = call(
        functools.partial(right_kernel, low), both, [SMEM, VMEM, VMEM] + [ANY] * 11, (VMEM, VMEM),
        [pltpu.VMEM((2, 9 * seg, NT), left.dtype), dma((2,)), dma((2, 3))], 9 * flops, NEAR_MIB, {1: 1, 2: 0},
    )(pos, kept(blocks), kept(acc), left, *behind, ahead, *pieces[8:14])
    acc, blocks = call(
        functools.partial(tail_kernel, low), both, [SMEM, VMEM, VMEM] + [ANY] * 6, (VMEM, VMEM),
        [tile, dma((2, 2))], 2 * flops, NEAR_MIB, {1: 1, 2: 0},
    )(pos, kept(blocks), kept(acc), *pieces[:6])
    parts = 2 * half // NT
    return call(
        rest_kernel, (total, pltpu.VMEM((parts, depth, NT), left.dtype)), [SMEM, VMEM, VMEM] + [ANY] * 16, (VMEM, VMEM),
        [pltpu.VMEM((parts, depth, NT), left.dtype), dma((parts,)), dma], 7 * flops, NEAR_MIB, {2: 0},
    )(pos, kept(blocks), kept(acc), *pieces)


def far(acc, tile, chunks, powers):
    depth = chunks[0].shape[1]
    rows = sum(chunk.shape[0] for chunk in chunks)
    low = powers[0].shape[1] if powers else 0
    out = pltpu.VMEM(acc.shape, acc.dtype), pltpu.VMEM(tile.shape, tile.dtype), jax.ShapeDtypeStruct((8, low + rows), jnp.float32)
    return call(
        functools.partial(far_kernel, low), out, [VMEM, VMEM] + [VMEM] * len(powers) + [ANY] * len(chunks), (VMEM, VMEM, VMEM),
        [pltpu.VMEM((rows, depth), chunks[0].dtype), pltpu.VMEM((rows, 128), jnp.float32),
         pltpu.SemaphoreType.DMA((len(chunks),))],
        2 * rows * depth * acc.shape[1], FAR_MIB, {0: 0, 1: 1},
    )(kept(acc), kept(tile), *powers, *chunks)


def scale(cols, acc, powers):
    rows, width = acc.shape
    return call(
        functools.partial(scale_kernel, cols), jax.ShapeDtypeStruct(acc.shape, jnp.float32), [VMEM] * 5, ANY,
        [pltpu.VMEM((rows // 128, 128, width), jnp.float32), pltpu.SemaphoreType.DMA((rows // 128,))],
        rows * width * 30, 12,
    )(kept(acc), *powers)


def per_device(left, right):
    width = right.shape[1]
    half = width // 2
    me, z = lax.axis_index("gy"), lax.axis_index("gx")
    pos = jnp.stack([me // (NX * NC), (me // NC) % NX, me % NC, z]).astype(jnp.int32)

    ahead = move(left, "z", False)
    behind, opposite, low = [], [], 0
    for i, size in enumerate(ROW_CHUNKS):
        behind.append(move(left[low:low + size], "z", True))
        opposite.append(move(behind[i], "z", True))
        low += size
    pieces = []
    for h, (a, b) in enumerate((("x", "y"), ("y", "x"))):
        line = jnp.concatenate(ring(right[:, h * half:(h + 1) * half], a), axis=0)
        for v in ring(line, b):
            pieces += [v, move(v, "core", True)]

    pieces = [v if i % 8 == 7 else apart(v) for i, v in enumerate(pieces)]
    acc, tile = near(pos, apart(left), [apart(v) for v in behind], apart(ahead), pieces)
    acc, tile, power = far(acc, tile, opposite[:-1], [])
    acc, tile, power = far(acc, tile, opposite[-1:], [power])
    return scale(width * NZ, acc, exchange(power))


def solution(mesh):
    placed = (P("gy", "gx"), P("gy", "gx"))
    return jax.shard_map(per_device, mesh=mesh, in_specs=placed, out_specs=P("gy", "gx"), check_vma=False)
```
